32 devices in a mesh: dp: 2 (over x), expert: 4 (over y, core), sample: 4 (over z).
Axes of the slice: x: 2, y: 2, z: 4, core: 2. Of those that a mesh axis runs over, the one named last changes fastest.
Arguments:
- tokens: bfloat16 [640, 4096], P(('dp', 'expert', 'sample')), may hold values from -6 to 6
- cotangent: bfloat16 [640, 4096], P(('dp', 'expert', 'sample')), may hold values from -6 to 6
- routes: int32 [640, 2], P(('dp', 'expert', 'sample')), may hold values from 0 to 7, all different within a row; in each aligned block of 20 rows (0 to 19, 20 to 39, ...) at most 6 rows name the same one
- gate_weights: float32 [640, 2], P(('dp', 'expert', 'sample')), may hold values from 0.1 to 1
- lengths: int32 [8, 4], P(('dp', 'expert'), 'sample'), may hold values from 1 to 20
- rewards: int32 [8, 4], P(('dp', 'expert'), 'sample'), may hold values from -48 to 48
- w_gate: bfloat16 [8, 8192, 4096], P('expert', ('dp', 'sample')), may hold values from -0.09375 to 0.09375
- w_up: bfloat16 [8, 8192, 4096], P('expert', ('dp', 'sample')), may hold values from -0.09375 to 0.09375
- w_down: bfloat16 [8, 8192, 4096], P('expert', ('dp', 'sample')), may hold values from -0.0625 to 0.0625
Outputs:
- grad_tokens: bfloat16 [640, 4096], P(('dp', 'expert', 'sample'))
- grad_w_gate: bfloat16 [8, 8192, 4096], P('expert', ('dp', 'sample'))
- grad_w_up: bfloat16 [8, 8192, 4096], P('expert', ('dp', 'sample'))
- grad_w_down: bfloat16 [8, 8192, 4096], P('expert', ('dp', 'sample'))
The draws below stay inside these ranges and needn't reach their ends.
Inputs may be any that keep to these rules, and one draw needn't show every extreme that they name: `routes`: each row names 2 different experts; among the rows of one device no expert is named by more than 6 rows, and in every draw some device's rows name some expert exactly 6 times.
All inputs are finite; a program needn't handle non-finite values.
Results may differ from the reference program's by a relative error of at most 0.025.
Values may be sent and summed in bfloat16 or wider, within the bound.
A program may use at most 192 MiB of HBM per device.

```python
import math
import jax
import jax.numpy as jnp
import numpy as np
from jax import lax

D = 4096
FF = 8192
EXPERTS = 8
TOP = 2
TOK_DEV = 20
CAP = 6
K = 4
PROMPTS = 8
TOKENS = 640
N_DP = 2
N_EXPERT = 4
N_SAMPLE = 4


def touch_ends(drawn, rng, low, top_value):
    longest = drawn.shape.index(max(drawn.shape))
    spots = []
    for shift in (0, 1):
        where = [jax.random.randint(jax.random.fold_in(rng, axis), (), 0, length) for axis, length in enumerate(drawn.shape)]
        where[longest] = (where[longest] + shift) % drawn.shape[longest]
        spots.append(tuple(where))
    return drawn.at[spots[0]].set(low).at[spots[1]].set(top_value)


def block_scale(rng, shape, pieces, smallest, top_value):
    def one(dim, parts):
        heights = jax.random.uniform(jax.random.fold_in(jax.random.fold_in(rng, 6), dim), (parts,), jnp.float32, smallest / len(pieces), top_value / len(pieces))
        return jnp.repeat(jnp.exp(heights), shape[dim] // parts).reshape((-1,) + (1,) * (len(shape) - dim - 1))

    loudness = one(*pieces[0])
    for cut in pieces[1:]:
        loudness = loudness * one(*cut)
    return loudness


def shared_out(rng, own, number, rows, count, top, most, skew):
    ranking = jax.random.permutation(rng, count)
    crowded, usual = portions_of(count, rows * top, most, skew, True), portions_of(count, rows * top, most, skew, False)
    places = jnp.arange(count)

    def named(sizes, offset_by):
        used = int((sizes > 0).sum())
        fixed = max(1, used // 4)
        passed = fixed + (places - fixed + offset_by * (used - fixed)) % max(1, count - fixed)
        return jnp.zeros((count,), jnp.int32).at[ranking[jnp.where(places < fixed, places, passed)]].set(jnp.asarray(sizes, jnp.int32))

    sizes = jnp.where(number % 4 == 0, named(crowded, number // 4), named(usual, number - number // 4 - 1))
    mixed = jax.random.permutation(jax.random.fold_in(own, 3), count)
    giver, receiver = mixed[0:count // 2 * 2:2], mixed[1:count // 2 * 2:2]
    margin = jnp.minimum(sizes[giver] - 1, most - sizes[receiver]) // 2
    margin = jnp.where((giver == ranking[0]) | (receiver == ranking[0]) | (sizes[receiver] == 0), 0, jnp.maximum(margin, 0))
    passed = jax.random.randint(jax.random.fold_in(own, 4), (count // 2,), 0, 1 << 20) % (margin + 1)
    sizes = sizes.at[giver].add(-passed).at[receiver].add(passed)
    labels = jnp.searchsorted(jnp.cumsum(sizes), jnp.arange(rows * top), side="right").astype(jnp.int32)
    grid = labels.reshape(top, rows).T
    grid = grid[jax.random.permutation(jax.random.fold_in(own, 1), rows)]
    offset_by = jax.random.randint(jax.random.fold_in(own, 2), (rows, 1), 0, top)
    return jnp.take_along_axis(grid, (jnp.arange(top)[None, :] + offset_by) % top, axis=1)


def portions_of(amount, total, bound, skew, full):
    weights = [(1 << 20) // math.isqrt(standing ** skew) + 1 for standing in range(1, amount + 1)]
    largest = bound if full else min(bound, max(-(-total // amount), total * weights[0] // sum(weights)))
    least = 1 if total - largest >= amount - 1 else 0
    holding, spare = [largest] + [least] * (amount - 1), total - largest - least * (amount - 1)
    while spare > 0:
        candidates = [i for i in range(1, amount) if holding[i] < largest] or [i for i in range(1, amount) if holding[i] < bound]
        whole, budget = sum([weights[i] for i in candidates]), spare
        for i in candidates:
            more = min(bound - holding[i], max(1, budget * weights[i] // whole), spare)
            holding[i] = holding[i] + more
            spare = spare - more
    return np.array(holding)


def centred(key, dims, spread, reach, shards=(), kind=jnp.bfloat16):
    gain = block_scale(key, dims, shards, -0.22, 0.18) if shards else 1.0
    array = jax.random.normal(key, dims, jnp.float32) * spread * gain
    return jnp.minimum(jnp.maximum(array, -reach), reach).astype(kind)


def setup_inputs(seed: int = 0) -> dict:
    streams_of = jax.random.split(jax.random.key(seed), 10)
    tokens = centred(streams_of[0], (TOKENS, D), 1.0, 6.0, ((0, 32),))
    cotangent = centred(streams_of[1], (TOKENS, D), 1.0, 6.0, ((0, 32),))
    routes_keys = jax.random.split(jax.random.fold_in(streams_of[2], 1), TOKENS // TOK_DEV)
    routes_turns = jax.random.permutation(jax.random.fold_in(streams_of[2], 3), TOKENS // TOK_DEV)
    routes = jax.vmap(lambda own, number: shared_out(jax.random.fold_in(streams_of[2], 2), own, number, TOK_DEV, EXPERTS, TOP, CAP, 2))(routes_keys, routes_turns).reshape((TOKENS, TOP))
    gate_weights = jnp.clip(0.1 + 0.9 * jax.random.uniform(streams_of[3], (TOKENS, TOP), jnp.float32) ** block_scale(streams_of[3], (TOKENS, TOP), ((0, 32),), -0.2, 0.2), 0.1, 1.0)
    lengths = touch_ends(jax.random.randint(streams_of[4], (PROMPTS, K), 1, TOK_DEV + 1), jax.random.fold_in(streams_of[4], 1), 1, TOK_DEV).astype(jnp.int32)
    rewards = touch_ends(jax.random.randint(streams_of[5], (PROMPTS, K), -48, 49), jax.random.fold_in(streams_of[5], 1), -48, 48).astype(jnp.int32)
    w_gate = centred(streams_of[6], (EXPERTS, FF, D), D ** -0.5, 0.09375, ((0, 4), (1, 8)))
    w_up = centred(streams_of[7], (EXPERTS, FF, D), D ** -0.5, 0.09375, ((0, 4), (1, 8)))
    w_down = centred(streams_of[8], (EXPERTS, FF, D), FF ** -0.5, 0.0625, ((0, 4), (1, 8)))
    return dict(tokens=tokens, cotangent=cotangent, routes=routes, gate_weights=gate_weights, lengths=lengths, rewards=rewards, w_gate=w_gate, w_up=w_up, w_down=w_down)


def silu_parts(pre_gate):
    gate_prob = jax.nn.sigmoid(pre_gate)
    return pre_gate * gate_prob, gate_prob * (1.0 + pre_gate * (1.0 - gate_prob))


def reference(tokens, cotangent, routes, gate_weights, lengths, rewards, w_gate, w_up, w_down):
    devices = N_DP * N_EXPERT * N_SAMPLE
    slices = N_DP * N_SAMPLE
    width_slice = FF // slices
    choices_per = routes.shape[1]
    reward = rewards.astype(jnp.float32) * 0.0625
    reward_total = jnp.sum(reward, axis=1, keepdims=True)
    advantage = reward - (reward_total - reward) / (K - 1)
    owner = jnp.arange(TOKENS, dtype=jnp.int32) // TOK_DEV
    position = jnp.arange(TOKENS, dtype=jnp.int32) % TOK_DEV
    live = position < lengths.reshape(-1)[owner]
    weight_row = jnp.where(live, -advantage.reshape(-1)[owner], jnp.zeros((), jnp.float32))
    pair_scale = (gate_weights * weight_row[:, None]).reshape(-1)
    pair_expert = routes.reshape(-1)
    pair_count = pair_expert.shape[0]
    limit = devices * CAP
    member = (pair_expert[:, None] == jnp.arange(EXPERTS, dtype=jnp.int32)[None, :]).astype(jnp.int32)
    order = jnp.cumsum(member, axis=0) - 1
    where_row = jnp.where(member > 0, order, limit).astype(jnp.int32)
    pair_ids = jnp.broadcast_to(jnp.arange(pair_count, dtype=jnp.int32)[:, None], member.shape)
    expert_ids = jnp.broadcast_to(jnp.arange(EXPERTS, dtype=jnp.int32)[None, :], member.shape)
    table = jnp.zeros((EXPERTS, limit), jnp.int32).at[expert_ids, where_row].set(pair_ids, mode="drop")
    filled = jnp.arange(limit, dtype=jnp.int32)[None, :] < jnp.sum(member, axis=0)[:, None]

    def one_expert(packed):
        pair_rows, valid, gate_rows, up_rows, down_rows = packed
        token_rows = pair_rows // choices_per
        inputs = tokens[token_rows]
        scale = jnp.where(valid, pair_scale[pair_rows], jnp.zeros((), jnp.float32))
        grads_out = (cotangent[token_rows].astype(jnp.float32) * scale[:, None]).astype(jnp.bfloat16)
        pre_gate = jnp.dot(inputs, gate_rows.T, preferred_element_type=jnp.float32)
        pre_up = jnp.dot(inputs, up_rows.T, preferred_element_type=jnp.float32)
        active, derivative = silu_parts(pre_gate)
        hidden = (active * pre_up).astype(jnp.bfloat16)
        grad_hidden = jnp.dot(grads_out, down_rows.T, preferred_element_type=jnp.float32)
        grad_gate = (grad_hidden * pre_up * derivative).astype(jnp.bfloat16)
        grad_up = (grad_hidden * active).astype(jnp.bfloat16)
        down_grad = jnp.dot(hidden.T, grads_out, preferred_element_type=jnp.float32).astype(jnp.bfloat16)
        gate_grad = jnp.dot(grad_gate.T, inputs, preferred_element_type=jnp.float32).astype(jnp.bfloat16)
        up_grad = jnp.dot(grad_up.T, inputs, preferred_element_type=jnp.float32).astype(jnp.bfloat16)

        def add_slice(index, total):
            first = (index * width_slice).astype(jnp.int32)
            piece_gate = lax.dynamic_slice_in_dim(grad_gate, first, width_slice, 1)
            piece_up = lax.dynamic_slice_in_dim(grad_up, first, width_slice, 1)
            block_gate = lax.dynamic_slice_in_dim(gate_rows, first, width_slice, 0)
            block_up = lax.dynamic_slice_in_dim(up_rows, first, width_slice, 0)
            part = jnp.dot(piece_gate, block_gate, preferred_element_type=jnp.float32) + jnp.dot(piece_up, block_up, preferred_element_type=jnp.float32)
            rounded = lax.optimization_barrier(part.astype(jnp.bfloat16))
            return total + rounded.astype(jnp.float32)

        row_total = lax.fori_loop(0, slices, add_slice, jnp.zeros((limit, D), jnp.float32))
        return gate_grad, up_grad, down_grad, row_total.astype(jnp.bfloat16)

    grad_gate_all, grad_up_all, grad_down_all, row_grads = lax.map(one_expert, (table, filled, w_gate, w_up, w_down))
    token_rows = (table // choices_per).reshape(-1)
    masked = jnp.where(filled.reshape(-1)[:, None], row_grads.reshape(-1, D).astype(jnp.float32), jnp.zeros((), jnp.float32))
    grad_tokens = jnp.zeros((TOKENS, D), jnp.float32).at[token_rows].add(masked).astype(jnp.bfloat16)
    return grad_tokens, grad_gate_all, grad_up_all, grad_down_all
```

```python
import functools

import jax
import jax.numpy as jnp
from jax import lax
from jax.experimental import pallas as pl
from jax.experimental.pallas import tpu as pltpu
from jax.sharding import PartitionSpec as P

CAP = 6
BF16 = jnp.bfloat16
F32 = jnp.float32
MESH = pl.DeviceIdType.MESH


def silu_parts(pre_gate):
    gate_prob = jax.nn.sigmoid(pre_gate)
    return (pre_gate * gate_prob, gate_prob * (1.0 + pre_gate * (1.0 - gate_prob)))


def expert_rows(inputs, grads_out, w_gate, w_up, w_down):
    pre_gate = jnp.einsum("rjcd,jfd->rjcf", inputs, w_gate, preferred_element_type=jnp.float32)
    pre_up = jnp.einsum("rjcd,jfd->rjcf", inputs, w_up, preferred_element_type=jnp.float32)
    active, derivative = silu_parts(pre_gate)
    hidden = (active * pre_up).astype(jnp.bfloat16)
    grad_hidden = jnp.einsum(
        "rjcd,jfd->rjcf", grads_out, w_down, preferred_element_type=jnp.float32
    )
    grad_gate = (grad_hidden * pre_up * derivative).astype(jnp.bfloat16)
    grad_up = (grad_hidden * active).astype(jnp.bfloat16)
    return (hidden, grad_gate, grad_up)


def weight_terms(inputs, grads_out, hidden, grad_gate, grad_up):
    term_gate = jnp.einsum("rjcf,rjcd->jfd", grad_gate, inputs, preferred_element_type=jnp.float32)
    term_up = jnp.einsum("rjcf,rjcd->jfd", grad_up, inputs, preferred_element_type=jnp.float32)
    term_down = jnp.einsum("rjcf,rjcd->jfd", hidden, grads_out, preferred_element_type=jnp.float32)
    return (term_gate, term_up, term_down)


def input_terms(grad_gate, grad_up, w_gate, w_up):
    from_gate = jnp.einsum("rjcf,jfd->rjcd", grad_gate, w_gate, preferred_element_type=jnp.float32)
    from_up = jnp.einsum("rjcf,jfd->rjcd", grad_up, w_up, preferred_element_type=jnp.float32)
    return from_gate + from_up


def send_sum(blocks, axis):
    count = lax.axis_size(axis)
    me = lax.axis_index(axis)
    total = lax.dynamic_index_in_dim(blocks, me, 0, keepdims=False).astype(jnp.float32)
    for step in range(1, count):
        outgoing = lax.dynamic_index_in_dim(blocks, (me + step) % count, 0, keepdims=False)
        perm = [(i, (i + step) % count) for i in range(count)]
        total = total + lax.ppermute(outgoing, axis, perm).astype(jnp.float32)
    return total.astype(jnp.bfloat16)


def local(tokens, cotangent, routes, gate_weights, lengths, rewards, w_gate, w_up, w_down):
    samples = lax.axis_size("sample")
    own_reward = rewards.astype(jnp.float32) * 0.0625
    reward_total = own_reward
    for step in range(1, samples):
        perm = [(i, (i + step) % samples) for i in range(samples)]
        reward_total = reward_total + lax.ppermute(own_reward, "sample", perm)
    advantage = own_reward - (reward_total - own_reward) / (samples - 1)
    token_count = tokens.shape[0]
    model_width = tokens.shape[1]
    choices_per = routes.shape[1]
    local_experts = w_gate.shape[0]
    expert_groups = lax.axis_size("expert")
    all_experts = local_experts * expert_groups
    positions = jnp.arange(token_count, dtype=jnp.int32)
    weight_row = jnp.where(positions < lengths[0, 0], -advantage[0, 0], jnp.zeros((), jnp.float32))
    pair_scale = (gate_weights * weight_row[:, None]).reshape(-1)
    pair_expert = routes.reshape(-1)
    member = (pair_expert[:, None] == jnp.arange(all_experts, dtype=jnp.int32)[None, :]).astype(
        jnp.int32
    )
    earlier = jnp.sum((jnp.cumsum(member, axis=0) - member) * member, axis=1)
    target = pair_expert * CAP + earlier
    slot_ids = jnp.arange(all_experts * CAP, dtype=jnp.int32)
    placed = target[:, None] == slot_ids[None, :]
    chosen = jnp.sum(
        placed.reshape(token_count, choices_per, -1).astype(jnp.float32), axis=1
    ).astype(jnp.bfloat16)
    slot_scale = jnp.sum(jnp.where(placed, pair_scale[:, None], jnp.zeros((), jnp.float32)), axis=0)
    sent_inputs = jnp.dot(chosen.T, tokens, preferred_element_type=jnp.float32).astype(jnp.bfloat16)
    sent_cotangent = jnp.dot(chosen.T, cotangent, preferred_element_type=jnp.float32)
    sent_grads = (sent_cotangent * slot_scale[:, None]).astype(jnp.bfloat16)
    layout = (expert_groups, local_experts, CAP, model_width)
    arrived_inputs, arrived_grads = (
        lax.all_to_all(
            sent_inputs.reshape(layout), "expert", split_axis=0, concat_axis=0, tiled=True
        ),
        lax.all_to_all(
            sent_grads.reshape(layout), "expert", split_axis=0, concat_axis=0, tiled=True
        ),
    )
    group_inputs, group_grads = (
        lax.all_gather(arrived_inputs, ("dp", "sample"), axis=0, tiled=True),
        lax.all_gather(arrived_grads, ("dp", "sample"), axis=0, tiled=True),
    )
    hidden, grad_gate, grad_up = expert_rows(group_inputs, group_grads, w_gate, w_up, w_down)
    term_gate, term_up, term_down = weight_terms(
        group_inputs, group_grads, hidden, grad_gate, grad_up
    )
    parts = input_terms(grad_gate, grad_up, w_gate, w_up).astype(jnp.bfloat16)
    dp_size = lax.axis_size("dp")
    parts = parts.reshape(dp_size, samples, all_experts * CAP, model_width)
    row_sums = send_sum(send_sum(parts, "dp"), "sample").reshape(layout)
    returned = lax.all_to_all(row_sums, "expert", split_axis=0, concat_axis=0, tiled=True)
    flat_back = returned.reshape(all_experts * CAP, model_width)
    grad_tokens = jnp.dot(chosen, flat_back, preferred_element_type=jnp.float32).astype(
        jnp.bfloat16
    )
    return (
        grad_tokens,
        term_gate.astype(jnp.bfloat16),
        term_up.astype(jnp.bfloat16),
        term_down.astype(jnp.bfloat16),
    )


NSUB = 4
NQ = 4
LANES = 128


def dot_nt(a, b):
    return lax.dot_general(a, b, (((1,), (1,)), ((), ())), preferred_element_type=F32)


def dot_nn(a, b):
    return lax.dot_general(a, b, (((1,), (0,)), ((), ())), preferred_element_type=F32)


def eye(n):
    rows = lax.broadcasted_iota(jnp.int32, (n, n), 0)
    cols = lax.broadcasted_iota(jnp.int32, (n, n), 1)
    return jnp.where(rows == cols, 1.0, 0.0).astype(BF16)


def pack_meta(routes, gate_weights, lengths, rewards, experts, per_group, ns, rows):
    tokens = routes.shape[0]
    z = lax.axis_index("sample")
    ids = jnp.arange(experts, dtype=jnp.int32)
    hit = routes[:, :, None] == ids[None, None, :]
    member = jnp.any(hit, axis=1)
    pos = jnp.arange(tokens, dtype=jnp.int32)
    before = (pos[None, :] < pos[:, None])[:, :, None] & member[None, :, :]
    rank = jnp.sum(before.astype(jnp.int32), axis=1)
    live = (pos < lengths[0, 0]).astype(F32)
    gate = jnp.sum(jnp.where(hit, gate_weights[:, :, None], 0.0), axis=1) * live[:, None]
    cap_line = ns * CAP
    slot = rank + (ids % per_group)[None, :] * cap_line + z * CAP + 1
    sub = jnp.arange(NSUB, dtype=jnp.int32)[:, None, None] * (per_group * cap_line)
    code = jnp.where(member[None], slot[None] + sub, 0).astype(F32)
    gate = jnp.broadcast_to(gate[None], code.shape)

    def lanes(a):
        a = jnp.transpose(a, (2, 0, 1)).reshape(experts // per_group, per_group, rows)
        return a

    both = jnp.concatenate([lanes(code), lanes(gate)], axis=1)
    both = both.reshape(-1, 4 * per_group, rows)
    reward = jnp.broadcast_to(
        rewards.astype(F32).reshape(1, 1, 1) * 0.0625, both.shape[:2] + (LANES - rows,)
    )
    return jnp.concatenate([both, reward], axis=2)


def fused_kernel(
    cfg,
    tok, cot, meta, wg, wu, wd,
    gt, h_out, gg_out, gu_out, x_out,
    buf, mbuf, r0, r1, r2, r3, xs, xq, acc, ht, gn, sel, sel_t, scol, wslot,
    z_send, z_recv, l_send, l_recv, d_recv, a_send, a_recv, b_send, b_recv,
    c_send, c_recv, e_send, e_recv, wsem, osem,
):
    ns, rows, cw, m, h, jl, cap_line = (
        cfg["ns"], cfg["rows"], cfg["cw"], cfg["m"], cfg["h"], cfg["jl"], cfg["cap_line"]
    )
    nk = 2 * NQ
    cq = NSUB * cw
    kl = ns * rows
    x = lax.axis_index("dp")
    ex = lax.axis_index("expert")
    z = lax.axis_index("sample")
    y = ex // 2
    c = ex % 2
    x1, y1 = x + (1 - c) * (1 - 2 * x), y + c * (1 - 2 * y)
    x2, y2 = x + c * (1 - 2 * x), y + (1 - c) * (1 - 2 * y)
    l0 = x * 2 + y
    l1 = x1 * 2 + y1
    l2 = x2 * 2 + y2
    l3 = (1 - x) * 2 + (1 - y)

    def dev(xx, yy, cc, zz):
        return {"dp": xx, "expert": yy * 2 + cc, "sample": zz}

    d1, d2, dc = dev(x1, y1, c, z), dev(x2, y2, c, z), dev(x, y, 1 - c, z)

    def zpeer(o):
        return (z + o) % ns

    def zsrc(o):
        return (z - o + ns) % ns

    barrier = pltpu.get_barrier_semaphore()
    peers = [d1, d2, dc] + [dev(x, y, c, zpeer(o)) for o in range(1, ns)]
    for p in peers:
        pl.semaphore_signal(barrier, inc=1, device_id=p, device_id_type=MESH)

    def load(mat, q, slot):
        return pltpu.make_async_copy(
            mat.at[:, :, pl.ds(pl.multiple_of(q * cq, cq), cq)], wslot.at[slot], wsem.at[slot]
        )

    load(wg, 0, 0).start()
    load(wu, 0, 1).start()
    load(wg, 1, 2).start()
    load(wu, 1, 3).start()
    load(wd, 0, 4).start()
    load(wd, 1, 5).start()

    for q in range(NQ):
        buf[q, c, l0, z] = tok[q]
        buf[NQ + q, c, l0, z] = cot[q]
    mbuf[c, l0, z] = meta[...]
    acc[...] = jnp.zeros_like(acc)
    pl.semaphore_wait(barrier, len(peers))

    def rc(src, dst, s, r, to):
        return pltpu.make_async_remote_copy(
            src_ref=src, dst_ref=dst, send_sem=s, recv_sem=r, device_id=to, device_id_type=MESH
        )

    def slab(k):
        return mbuf if isinstance(k, int) and k == nk else buf.at[k]

    def src_of(k):
        if isinstance(k, int) and k == nk:
            return meta
        return tok.at[k] if k < NQ else cot.at[k - NQ]

    def z_copy(k, o):
        to = dev(x, y, c, zpeer(o))
        return rc(src_of(k), slab(k).at[c, l0, z], z_send.at[k, o], z_recv.at[k, o], to)

    def z_wait(k):
        for o in range(1, ns):
            b = slab(k).at[c, l0, zsrc(o)]
            rc(b, b, z_send.at[k, o], z_recv.at[k, o], d1).wait_recv()

    def line(k, cc, ll, si, r, to):
        b = slab(k).at[cc, ll]
        return rc(b, b, l_send.at[k, si], r, to)

    def stage_a(k):
        z_wait(k)
        line(k, c, l0, 0, l_recv.at[k, 0], d1).start()
        line(k, c, l0, 1, l_recv.at[k, 1], d2).start()
        line(k, c, l0, 2, d_recv.at[k, l0], dc).start()

    def stage_b(k):
        line(k, c, l1, 0, l_recv.at[k, 0], d1).wait_recv()
        line(k, c, l1, 3, l_recv.at[k, 2], d2).start()
        line(k, c, l1, 4, d_recv.at[k, l1], dc).start()

    def stage_c(k):
        line(k, c, l2, 1, l_recv.at[k, 1], d2).wait_recv()
        line(k, c, l2, 5, d_recv.at[k, l2], dc).start()
        line(k, c, l3, 3, l_recv.at[k, 2], d2).wait_recv()
        line(k, c, l3, 6, d_recv.at[k, l3], dc).start()

    def stage_d(k):
        for ll in range(4):
            line(k, 1 - c, ll, 2, d_recv.at[k, ll], dc).wait_recv()

    def drain(k):
        for i in range(7):
            line(k, c, l0, i, l_recv.at[k, 0], d1).wait_send()

    for k in [nk] + list(range(nk)):
        for o in range(1, ns):
            z_copy(k, o).start()

    def build(g):
        mz = [mbuf[g // 4, g % 4, zz, ex // 2] for zz in range(ns)]
        lane = lax.broadcasted_iota(jnp.int32, (4 * jl, LANES), 1)
        rew = [
            jnp.sum(jnp.where(lane == LANES - 1, b, 0.0), axis=1, keepdims=True) for b in mz
        ]
        total = rew[0]
        for r in rew[1:]:
            total = total + r
        wide = -(-kl // LANES) * LANES
        vec = jnp.zeros((2 * jl, wide), F32)
        for zz in range(ns):
            adv = rew[zz] - (total - rew[zz]) / (ns - 1)
            b = jnp.where(lane < rows, mz[zz], 0.0)
            b = jnp.where(c == 1, b[2 * jl :], b[: 2 * jl])
            kind = lax.broadcasted_iota(jnp.int32, (2 * jl, LANES), 0)
            b = jnp.where(kind >= jl, b * (-adv[: 2 * jl]), b)
            b = jnp.concatenate([b, jnp.zeros((2 * jl, wide - LANES), F32)], axis=1)
            vec = vec + (pltpu.roll(b, zz * rows, 1) if zz else b)
        vec = vec[:, :kl]
        slots = NSUB * jl * cap_line
        ids = lax.broadcasted_iota(jnp.int32, (slots, kl), 0).astype(F32) + 1.0
        one = jnp.zeros((slots, kl), F32)
        scale = jnp.zeros((slots, kl), F32)
        for j in range(jl):
            same = ids == vec[j : j + 1]
            one = jnp.where(same, 1.0, one)
            scale = jnp.where(same, vec[jl + j : jl + j + 1], scale)
        one = one.astype(BF16)
        sel[g] = one
        scol[g] = jnp.sum(scale, axis=1, keepdims=True)
        sel_t[g] = dot_nt(eye(kl), one).astype(BF16)

    def select(k, scaled):
        def body(g, _):
            rowsv = buf[k, g // 4, g % 4].reshape(kl, cw)
            out = dot_nn(sel[g], rowsv)
            if scaled:
                out = out * scol[g]
            at = pl.ds(pl.multiple_of(g * cap_line, cap_line), cap_line)
            for s in range(NSUB):
                for j in range(jl):
                    r = (s * jl + j) * cap_line
                    xq[j, at, s * cw : (s + 1) * cw] = out[r : r + cap_line]
            return 0

        lax.fori_loop(0, 8, body, 0)
        xs[k] = xq[...].astype(BF16)

    def accumulate(i, slot, k):
        half = h // 2

        def body(t, _):
            j = t // 2
            r = pl.ds(pl.multiple_of((t % 2) * half, half), half)
            acc[i, j, r] += dot_nt(wslot[slot, j, r], xs[k, j])
            return 0

        lax.fori_loop(0, 2 * jl, body, 0)

    def wait_w(slot):
        load(wg, 0, slot).wait()

    def step(i):
        @pl.when(i < nk)
        def _():
            stage_a(i)

        @pl.when((i >= 1) & (i < nk + 1))
        def _():
            stage_b(i - 1)

        @pl.when((i >= 2) & (i < nk + 2))
        def _():
            stage_c(i - 2)

        @pl.when(i >= 3)
        def _():
            stage_d(i - 3)

    stage_a(nk)
    step(0)
    stage_b(nk)
    step(1)
    stage_c(nk)
    step(2)
    stage_d(nk)
    lax.fori_loop(0, 8, lambda g, _: (build(g), 0)[1], 0)

    def token_chunk(q, _):
        step(q + 3)
        select(q, False)
        s = 2 * (q % 2)
        wait_w(s)
        accumulate(0, s, q)
        wait_w(s + 1)
        accumulate(1, s + 1, q)

        @pl.when(q < NQ - 2)
        def _():
            load(wg, q + 2, s).start()
            load(wu, q + 2, s + 1).start()

        return 0

    lax.fori_loop(0, NQ, token_chunk, 0)

    def cot_chunk(q, _):
        step(q + NQ + 3)
        select(q + NQ, True)
        s = 4 + q % 2
        wait_w(s)
        accumulate(2, s, q + NQ)

        @pl.when(q < NQ - 2)
        def _():
            load(wd, q + 2, s).start()

        @pl.when(q == NQ - 2)
        def _():
            load(wg, 1, s).start()

        @pl.when(q == NQ - 1)
        def _():
            load(wu, 1, s).start()

        return 0

    lax.fori_loop(0, NQ, cot_chunk, 0)

    def finish(t, _):
        tile = h // 4
        j = t // 4
        r = pl.ds(pl.multiple_of((t % 4) * tile, tile), tile)
        g, u, gh = acc[0, j, r], acc[1, j, r], acc[2, j, r]
        act, der = silu_parts(g)
        ht[0, j, r] = (act * u).astype(BF16)
        ht[1, j, r] = (gh * u * der).astype(BF16)
        ht[2, j, r] = (gh * act).astype(BF16)
        return 0

    lax.fori_loop(0, 4 * jl, finish, 0)

    def turn(t, _):
        gn[t // jl, t % jl] = dot_nt(eye(m), ht[1 + t // jl, t % jl]).astype(BF16)
        return 0

    lax.fori_loop(0, 2 * jl, turn, 0)
    outs = [
        pltpu.make_async_copy(ht.at[0], h_out, osem.at[0]),
        pltpu.make_async_copy(ht.at[1], gg_out, osem.at[1]),
        pltpu.make_async_copy(ht.at[2], gu_out, osem.at[2]),
        pltpu.make_async_copy(xs, x_out, osem.at[3]),
    ]
    for o in outs:
        o.start()

    def drain_all(k, _):
        drain(k)
        return 0

    lax.fori_loop(0, nk, drain_all, 0)
    drain(nk)

    def parts(i):
        q = NQ - 1 - i
        s = (2 - 2 * i + 12) % 6

        @pl.when(i >= 2)
        def _():
            wait_w(s)
            wait_w(s + 1)

        def body(j, _):
            xq[j] = dot_nn(gn[0, j], wslot[s, j]) + dot_nn(gn[1, j], wslot[s + 1, j])
            return 0

        lax.fori_loop(0, jl, body, 0)

        @pl.when(i == 0)
        def _():
            load(wg, 0, s).start()
            load(wu, 0, s + 1).start()

        def back(g, _):
            at = pl.ds(pl.multiple_of(g * cap_line, cap_line), cap_line)
            pieces = [
                xq[j, at, sb * cw : (sb + 1) * cw] for sb in range(NSUB) for j in range(jl)
            ]
            v = jnp.concatenate(pieces, axis=0).astype(BF16)
            o = dot_nn(sel_t[g], v).astype(BF16)
            buf[q, g // 4, g % 4] = o.reshape(ns, rows, cw)
            return 0

        lax.fori_loop(0, 8, back, 0)
        send_core(q).start()

    def send_core(q):
        return rc(buf.at[q, 1 - c], r0.at[q], a_send.at[q], a_recv.at[q], dc)

    def send_far(q, i):
        return rc(
            buf.at[q, c, (l2, l3)[i]], r1.at[q, i], b_send.at[q, i], b_recv.at[q, i], d2
        )

    def send_near(q):
        return rc(buf.at[q, c, l1], r2.at[q], c_send.at[q], c_recv.at[q], d1)

    def send_z(q, o):
        to = dev(x, y, c, zpeer(o))
        return rc(buf.at[q, c, l0, zpeer(o)], r3.at[q, o], e_send.at[q, o], e_recv.at[q, o], to)

    def s1(q):
        send_core(q).wait_recv()
        for i, ll in ((0, l2), (1, l3)):
            buf[q, c, ll] = (buf[q, c, ll].astype(F32) + r0[q, ll].astype(F32)).astype(BF16)
            send_far(q, i).start()
        for ll in (l0, l1):
            buf[q, c, ll] = (buf[q, c, ll].astype(F32) + r0[q, ll].astype(F32)).astype(BF16)

    def s2(q):
        send_far(q, 1).wait_recv()
        buf[q, c, l1] = (buf[q, c, l1].astype(F32) + r1[q, 1].astype(F32)).astype(BF16)
        send_near(q).start()
        send_far(q, 0).wait_recv()
        buf[q, c, l0] = (buf[q, c, l0].astype(F32) + r1[q, 0].astype(F32)).astype(BF16)

    def s3(q):
        send_near(q).wait_recv()
        buf[q, c, l0] = (buf[q, c, l0].astype(F32) + r2[q].astype(F32)).astype(BF16)
        for o in range(1, ns):
            send_z(q, o).start()

    def s4(q):
        total = buf[q, c, l0, z].astype(F32)
        for o in range(1, ns):
            send_z(q, o).wait_recv()
            total = total + r3[q, o].astype(F32)
        gt[q] = total.astype(BF16)

    lags = cfg["lags"]

    def back_step(i, _):
        @pl.when(i < NQ)
        def _():
            parts(i)

        for fn, lag in zip((s1, s2, s3, s4), lags):

            @pl.when((i >= lag) & (i < lag + NQ))
            def _():
                fn(NQ - 1 - (i - lag))

        return 0

    lax.fori_loop(0, NQ + lags[-1], back_step, 0)

    def finish_sends(q, _):
        send_core(q).wait_send()
        send_far(q, 0).wait_send()
        send_far(q, 1).wait_send()
        send_near(q).wait_send()
        for o in range(1, ns):
            send_z(q, o).wait_send()
        return 0

    lax.fori_loop(0, NQ, finish_sends, 0)
    for k in [nk] + list(range(nk)):
        for o in range(1, ns):
            z_copy(k, o).wait_send()
    for o in outs:
        o.wait()


def weight_kernel(ht, gg, gu, xr, gr, o_gate, o_up, o_down):
    o_gate[0] = dot_nn(gg[0], xr[0, 0]).astype(BF16)
    o_up[0] = dot_nn(gu[0], xr[0, 0]).astype(BF16)
    o_down[0] = dot_nn(ht[0], gr[0, 0]).astype(BF16)


def fused(tokens, cotangent, routes, gate_weights, lengths, rewards, w_gate, w_up, w_down):
    ns = lax.axis_size("sample")
    t, d = tokens.shape
    jl, h, _ = w_gate.shape
    experts = jl * lax.axis_size("expert")
    rows = NSUB * t
    cw = d // (NSUB * NQ)
    cq = NSUB * cw
    cap_line = ns * CAP
    lines = 4
    m = 2 * lines * cap_line
    nk = 2 * NQ
    kl = ns * rows
    slots = NSUB * jl * cap_line
    cfg = dict(
        ns=ns, rows=rows, cw=cw, m=m, h=h, jl=jl, cap_line=cap_line, lags=(1, 3, 4, 6)
    )

    def fold(a):
        return a.reshape(t, NQ, NSUB, cw).transpose(1, 2, 0, 3).reshape(NQ, rows, cw)

    meta = pack_meta(routes, gate_weights, lengths, rewards, experts, jl, ns, rows)
    vmem = pl.BlockSpec(memory_space=pltpu.VMEM)
    hbm = pl.BlockSpec(memory_space=pltpu.HBM)
    dma = pltpu.SemaphoreType.DMA
    block = (rows, cw)
    back, ht, gg, gu, xs = pl.pallas_call(
        functools.partial(fused_kernel, cfg),
        name="gather_experts_scatter",
        out_shape=(
            jax.ShapeDtypeStruct((NQ,) + block, BF16),
            jax.ShapeDtypeStruct((jl, h, m), BF16),
            jax.ShapeDtypeStruct((jl, h, m), BF16),
            jax.ShapeDtypeStruct((jl, h, m), BF16),
            jax.ShapeDtypeStruct((nk, jl, m, cq), BF16),
        ),
        in_specs=[vmem] * 3 + [hbm] * 3,
        out_specs=(vmem, hbm, hbm, hbm, hbm),
        scratch_shapes=[
            pltpu.VMEM((nk, 2, lines, ns) + block, BF16),
            pltpu.VMEM((2, lines, ns) + meta.shape, F32),
            pltpu.VMEM((NQ, lines, ns) + block, BF16),
            pltpu.VMEM((NQ, 2, ns) + block, BF16),
            pltpu.VMEM((NQ, ns) + block, BF16),
            pltpu.VMEM((NQ, ns) + block, BF16),
            pltpu.VMEM((nk, jl, m, cq), BF16),
            pltpu.VMEM((jl, m, cq), F32),
            pltpu.VMEM((3, jl, h, m), F32),
            pltpu.VMEM((3, jl, h, m), BF16),
            pltpu.VMEM((2, jl, m, h), BF16),
            pltpu.VMEM((2 * lines, slots, kl), BF16),
            pltpu.VMEM((2 * lines, kl, slots), BF16),
            pltpu.VMEM((2 * lines, slots, 1), F32),
            pltpu.VMEM((6, jl, h, cq), BF16),
            dma((nk + 1, ns)), dma((nk + 1, ns)), dma((nk + 1, 7)), dma((nk + 1, 3)),
            dma((nk + 1, 4)), dma((NQ,)), dma((NQ,)), dma((NQ, 2)), dma((NQ, 2)),
            dma((NQ,)), dma((NQ,)), dma((NQ, ns)), dma((NQ, ns)), dma((6,)), dma((4,)),
        ],
        compiler_params=pltpu.CompilerParams(
            collective_id=0, has_side_effects=True, vmem_limit_bytes=67043328
        ),
    )(fold(tokens), fold(cotangent), meta, w_gate, w_up, w_down)

    full = pl.BlockSpec((1, h, m), lambda j, q: (j, 0, 0))
    out = pl.BlockSpec((1, h, cq), lambda j, q: (j, 0, q))
    shape = jax.ShapeDtypeStruct(w_gate.shape, BF16)
    g_gate, g_up, g_down = pl.pallas_call(
        weight_kernel,
        name="weight_grads",
        grid=(jl, NQ),
        out_shape=(shape, shape, shape),
        in_specs=[
            full, full, full,
            pl.BlockSpec((1, 1, m, cq), lambda j, q: (q, j, 0, 0)),
            pl.BlockSpec((1, 1, m, cq), lambda j, q: (NQ + q, j, 0, 0)),
        ],
        out_specs=(out, out, out),
        compiler_params=pltpu.CompilerParams(vmem_limit_bytes=48 * 1024 * 1024),
    )(ht, gg, gu, xs, xs)
    grad_tokens = back.reshape(NQ, NSUB, t, cw).transpose(2, 0, 1, 3).reshape(t, d)
    return grad_tokens, g_gate, g_up, g_down


def covered(mesh, tokens_shape, w_shape, rewards_shape):
    nx, ne, ns = (mesh.shape[a] for a in ("dp", "expert", "sample"))
    t = tokens_shape[0] // (nx * ne * ns)
    d = tokens_shape[1]
    h = w_shape[1] // (nx * ns)
    prompt_one = rewards_shape == (nx * ne, ns)
    return (
        nx == 2
        and ne == 4
        and w_shape[0] == 2 * ne
        and prompt_one
        and ns > 1
        and (ns * CAP) % 8 == 0
        and (NSUB * t) % 16 == 0
        and NSUB * t < LANES
        and d % (NSUB * NQ * LANES) == 0
        and h % 1024 == 0
        and ns * t * d * h <= 80 * 4096 * 1024
    )


def solution(mesh):
    in_specs = (
        P(("dp", "expert", "sample"), None),
        P(("dp", "expert", "sample"), None),
        P(("dp", "expert", "sample"), None),
        P(("dp", "expert", "sample"), None),
        P(("dp", "expert"), "sample"),
        P(("dp", "expert"), "sample"),
        P("expert", ("dp", "sample"), None),
        P("expert", ("dp", "sample"), None),
        P("expert", ("dp", "sample"), None),
    )
    out_specs = (
        P(("dp", "expert", "sample"), None),
        P("expert", ("dp", "sample"), None),
        P("expert", ("dp", "sample"), None),
        P("expert", ("dp", "sample"), None),
    )

    def run(*args):
        fits = covered(mesh, args[0].shape, args[6].shape, args[5].shape)
        body = fused if fits else local
        return jax.shard_map(
            body, mesh=mesh, in_specs=in_specs, out_specs=out_specs, check_vma=False
        )(*args)

    return run
```

```python
import functools

import jax
import jax.numpy as jnp
from jax import lax
from jax.experimental import pallas as pl
from jax.experimental.pallas import tpu as pltpu
from jax.sharding import PartitionSpec as P

CAP = 6
BF16 = jnp.bfloat16
F32 = jnp.float32
MESH = pl.DeviceIdType.MESH


def silu_parts(pre_gate):
    gate_prob = jax.nn.sigmoid(pre_gate)
    return (pre_gate * gate_prob, gate_prob * (1.0 + pre_gate * (1.0 - gate_prob)))


def expert_rows(inputs, grads_out, w_gate, w_up, w_down):
    pre_gate = jnp.einsum("rjcd,jfd->rjcf", inputs, w_gate, preferred_element_type=jnp.float32)
    pre_up = jnp.einsum("rjcd,jfd->rjcf", inputs, w_up, preferred_element_type=jnp.float32)
    active, derivative = silu_parts(pre_gate)
    hidden = (active * pre_up).astype(jnp.bfloat16)
    grad_hidden = jnp.einsum(
        "rjcd,jfd->rjcf", grads_out, w_down, preferred_element_type=jnp.float32
    )
    grad_gate = (grad_hidden * pre_up * derivative).astype(jnp.bfloat16)
    grad_up = (grad_hidden * active).astype(jnp.bfloat16)
    return (hidden, grad_gate, grad_up)


def weight_terms(inputs, grads_out, hidden, grad_gate, grad_up):
    term_gate = jnp.einsum("rjcf,rjcd->jfd", grad_gate, inputs, preferred_element_type=jnp.float32)
    term_up = jnp.einsum("rjcf,rjcd->jfd", grad_up, inputs, preferred_element_type=jnp.float32)
    term_down = jnp.einsum("rjcf,rjcd->jfd", hidden, grads_out, preferred_element_type=jnp.float32)
    return (term_gate, term_up, term_down)


def input_terms(grad_gate, grad_up, w_gate, w_up):
    from_gate = jnp.einsum("rjcf,jfd->rjcd", grad_gate, w_gate, preferred_element_type=jnp.float32)
    from_up = jnp.einsum("rjcf,jfd->rjcd", grad_up, w_up, preferred_element_type=jnp.float32)
    return from_gate + from_up


def send_sum(blocks, axis):
    count = lax.axis_size(axis)
    me = lax.axis_index(axis)
    total = lax.dynamic_index_in_dim(blocks, me, 0, keepdims=False).astype(jnp.float32)
    for step in range(1, count):
        outgoing = lax.dynamic_index_in_dim(blocks, (me + step) % count, 0, keepdims=False)
        perm = [(i, (i + step) % count) for i in range(count)]
        total = total + lax.ppermute(outgoing, axis, perm).astype(jnp.float32)
    return total.astype(jnp.bfloat16)


def local(tokens, cotangent, routes, gate_weights, lengths, rewards, w_gate, w_up, w_down):
    samples = lax.axis_size("sample")
    own_reward = rewards.astype(jnp.float32) * 0.0625
    reward_total = own_reward
    for step in range(1, samples):
        perm = [(i, (i + step) % samples) for i in range(samples)]
        reward_total = reward_total + lax.ppermute(own_reward, "sample", perm)
    advantage = own_reward - (reward_total - own_reward) / (samples - 1)
    token_count = tokens.shape[0]
    model_width = tokens.shape[1]
    choices_per = routes.shape[1]
    local_experts = w_gate.shape[0]
    expert_groups = lax.axis_size("expert")
    all_experts = local_experts * expert_groups
    positions = jnp.arange(token_count, dtype=jnp.int32)
    weight_row = jnp.where(positions < lengths[0, 0], -advantage[0, 0], jnp.zeros((), jnp.float32))
    pair_scale = (gate_weights * weight_row[:, None]).reshape(-1)
    pair_expert = routes.reshape(-1)
    member = (pair_expert[:, None] == jnp.arange(all_experts, dtype=jnp.int32)[None, :]).astype(
        jnp.int32
    )
    earlier = jnp.sum((jnp.cumsum(member, axis=0) - member) * member, axis=1)
    target = pair_expert * CAP + earlier
    slot_ids = jnp.arange(all_experts * CAP, dtype=jnp.int32)
    placed = target[:, None] == slot_ids[None, :]
    chosen = jnp.sum(
        placed.reshape(token_count, choices_per, -1).astype(jnp.float32), axis=1
    ).astype(jnp.bfloat16)
    slot_scale = jnp.sum(jnp.where(placed, pair_scale[:, None], jnp.zeros((), jnp.float32)), axis=0)
    sent_inputs = jnp.dot(chosen.T, tokens, preferred_element_type=jnp.float32).astype(jnp.bfloat16)
    sent_cotangent = jnp.dot(chosen.T, cotangent, preferred_element_type=jnp.float32)
    sent_grads = (sent_cotangent * slot_scale[:, None]).astype(jnp.bfloat16)
    layout = (expert_groups, local_experts, CAP, model_width)
    arrived_inputs, arrived_grads = (
        lax.all_to_all(
            sent_inputs.reshape(layout), "expert", split_axis=0, concat_axis=0, tiled=True
        ),
        lax.all_to_all(
            sent_grads.reshape(layout), "expert", split_axis=0, concat_axis=0, tiled=True
        ),
    )
    group_inputs, group_grads = (
        lax.all_gather(arrived_inputs, ("dp", "sample"), axis=0, tiled=True),
        lax.all_gather(arrived_grads, ("dp", "sample"), axis=0, tiled=True),
    )
    hidden, grad_gate, grad_up = expert_rows(group_inputs, group_grads, w_gate, w_up, w_down)
    term_gate, term_up, term_down = weight_terms(
        group_inputs, group_grads, hidden, grad_gate, grad_up
    )
    parts = input_terms(grad_gate, grad_up, w_gate, w_up).astype(jnp.bfloat16)
    dp_size = lax.axis_size("dp")
    parts = parts.reshape(dp_size, samples, all_experts * CAP, model_width)
    row_sums = send_sum(send_sum(parts, "dp"), "sample").reshape(layout)
    returned = lax.all_to_all(row_sums, "expert", split_axis=0, concat_axis=0, tiled=True)
    flat_back = returned.reshape(all_experts * CAP, model_width)
    grad_tokens = jnp.dot(chosen, flat_back, preferred_element_type=jnp.float32).astype(
        jnp.bfloat16
    )
    return (
        grad_tokens,
        term_gate.astype(jnp.bfloat16),
        term_up.astype(jnp.bfloat16),
        term_down.astype(jnp.bfloat16),
    )


NSUB = 4
NQ = 4
LANES = 128
AHEAD = (2, 4, 5)
LOOK = 2


def dot_nt(a, b):
    return lax.dot_general(a, b, (((1,), (1,)), ((), ())), preferred_element_type=F32)


def dot_nn(a, b):
    return lax.dot_general(a, b, (((1,), (0,)), ((), ())), preferred_element_type=F32)


def eye(n):
    rows = lax.broadcasted_iota(jnp.int32, (n, n), 0)
    cols = lax.broadcasted_iota(jnp.int32, (n, n), 1)
    return jnp.where(rows == cols, 1.0, 0.0).astype(BF16)


def pack_meta(routes, gate_weights, lengths, rewards, experts, jl, cap_line, z):
    t = routes.shape[1]
    eid = lax.broadcasted_iota(jnp.int32, (experts, t), 0)
    live = lax.broadcasted_iota(jnp.int32, (1, t), 1) < lengths
    member = jnp.zeros((experts, t), F32)
    gate = jnp.zeros((experts, t), F32)
    for k in range(routes.shape[0]):
        hit = routes[k : k + 1] == eid
        member = jnp.where(hit, 1.0, member)
        gate = jnp.where(hit & live, gate_weights[k : k + 1], gate)
    before = lax.broadcasted_iota(jnp.int32, (t, t), 0) < lax.broadcasted_iota(jnp.int32, (t, t), 1)
    rank = dot_nn(member.astype(BF16), jnp.where(before, 1.0, 0.0).astype(BF16))
    base = ((eid % jl) * cap_line + z * CAP + 1).astype(F32)
    code = jnp.where(member > 0.0, rank + base, 0.0)
    reward = rewards.astype(F32) * 0.0625
    lanes = lax.broadcasted_iota(jnp.int32, (experts, LANES), 1)

    def spread(a, step):
        a = jnp.concatenate([a, jnp.zeros((experts, LANES - t), F32)], axis=1)
        out = a
        for sub in range(1, NSUB):
            moved = pltpu.roll(a, sub * t, 1)
            out = out + (jnp.where(moved > 0.0, moved + sub * step, 0.0) if step else moved)
        return jnp.where(lanes == LANES - 1, reward, out)

    return spread(code, float(jl * cap_line)), spread(gate, 0.0)


def place(rows, t, sub):
    r = lax.broadcasted_iota(jnp.int32, (rows, t), 0)
    i = lax.broadcasted_iota(jnp.int32, (rows, t), 1)
    return jnp.where(r == i + sub * t, 1.0, 0.0).astype(BF16)


def take(rows, t, sub):
    r = lax.broadcasted_iota(jnp.int32, (t, rows), 1)
    i = lax.broadcasted_iota(jnp.int32, (t, rows), 0)
    return jnp.where(r == i + sub * t, 1.0, 0.0).astype(BF16)


def fused_kernel(
    cfg,
    tok, cot, routes, gates, lengths, rewards, wg, wu, wd,
    gt, h_out, gg_out, gu_out, x_out,
    buf, mbuf, r0, r1, r2, r3, xs, xq, acc, ht, gn, sel, sel_t, scol, wslot,
    z_send, z_recv, l_send, l_recv, d_recv, a_send, a_recv, b_send, b_recv,
    c_send, c_recv, e_send, e_recv, wsem, osem,
):
    ns, rows, cw, m, h, jl, cap_line = (
        cfg["ns"], cfg["rows"], cfg["cw"], cfg["m"], cfg["h"], cfg["jl"], cfg["cap_line"]
    )
    nk = 2 * NQ
    cq = NSUB * cw
    kl = ns * rows
    x = lax.axis_index("dp")
    ex = lax.axis_index("expert")
    z = lax.axis_index("sample")
    y = ex // 2
    c = ex % 2
    x1, y1 = x + (1 - c) * (1 - 2 * x), y + c * (1 - 2 * y)
    x2, y2 = x + c * (1 - 2 * x), y + (1 - c) * (1 - 2 * y)
    l0 = x * 2 + y
    l1 = x1 * 2 + y1
    l2 = x2 * 2 + y2
    l3 = (1 - x) * 2 + (1 - y)

    def dev(xx, yy, cc, zz):
        return {"dp": xx, "expert": yy * 2 + cc, "sample": zz}

    d1, d2, dc = dev(x1, y1, c, z), dev(x2, y2, c, z), dev(x, y, 1 - c, z)

    def zpeer(o):
        return (z + o) % ns

    def zsrc(o):
        return (z - o + ns) % ns

    barrier = pltpu.get_barrier_semaphore()
    peers = [d1, d2, dc] + [dev(x, y, c, zpeer(o)) for o in range(1, ns)]
    for p in peers:
        pl.semaphore_signal(barrier, inc=1, device_id=p, device_id_type=MESH)

    def load(mat, q, slot):
        return pltpu.make_async_copy(
            mat.at[:, :, pl.ds(pl.multiple_of(q * cq, cq), cq)], wslot.at[slot], wsem.at[slot]
        )

    load(wg, 0, 0).start()
    load(wu, 0, 1).start()
    load(wg, 1, 2).start()
    load(wu, 1, 3).start()
    load(wd, 0, 4).start()
    load(wd, 1, 5).start()

    t = tok.shape[0]
    spots = [place(rows, t, sub) for sub in range(NSUB)]

    def fold(k):
        ref, q = (tok, k) if k < NQ else (cot, k - NQ)
        out = jnp.zeros((rows, cw), F32)
        for sub in range(NSUB):
            at = q * cq + sub * cw
            out = out + dot_nn(spots[sub], ref[:, at : at + cw])
        buf[k, c, l0, z] = out.astype(BF16)

    code, gate = pack_meta(
        routes[...], gates[...], lengths[...], rewards[...], mbuf.shape[4], jl, cap_line, z
    )
    mbuf[c, l0, z, 0] = code
    mbuf[c, l0, z, 1] = gate
    for k in range(LOOK):
        fold(k)
    pl.semaphore_wait(barrier, len(peers))

    def rc(src, dst, s, r, to):
        return pltpu.make_async_remote_copy(
            src_ref=src, dst_ref=dst, send_sem=s, recv_sem=r, device_id=to, device_id_type=MESH
        )

    def slab(k):
        return mbuf if isinstance(k, int) and k == nk else buf.at[k]

    def z_copy(k, o):
        b = slab(k).at[c, l0, z]
        return rc(b, b, z_send.at[k, o], z_recv.at[k, o], dev(x, y, c, zpeer(o)))

    def z_start(k):
        for o in range(1, ns):
            z_copy(k, o).start()

    def z_wait(k):
        for o in range(1, ns):
            b = slab(k).at[c, l0, zsrc(o)]
            rc(b, b, z_send.at[k, o], z_recv.at[k, o], d1).wait_recv()

    def line(k, cc, ll, si, r, to):
        b = slab(k).at[cc, ll]
        return rc(b, b, l_send.at[k, si], r, to)

    def stage_a(k):
        z_wait(k)
        line(k, c, l0, 0, l_recv.at[k, 0], d1).start()
        line(k, c, l0, 1, l_recv.at[k, 1], d2).start()
        line(k, c, l0, 2, d_recv.at[k, l0], dc).start()

    def stage_b(k):
        line(k, c, l1, 0, l_recv.at[k, 0], d1).wait_recv()
        line(k, c, l1, 3, l_recv.at[k, 2], d2).start()
        line(k, c, l1, 4, d_recv.at[k, l1], dc).start()

    def stage_c(k):
        line(k, c, l2, 1, l_recv.at[k, 1], d2).wait_recv()
        line(k, c, l2, 5, d_recv.at[k, l2], dc).start()
        line(k, c, l3, 3, l_recv.at[k, 2], d2).wait_recv()
        line(k, c, l3, 6, d_recv.at[k, l3], dc).start()

    def stage_d(k):
        for ll in range(4):
            line(k, 1 - c, ll, 2, d_recv.at[k, ll], dc).wait_recv()

    def drain(k):
        for i in range(7):
            line(k, c, l0, i, l_recv.at[k, 0], d1).wait_send()
        for o in range(1, ns):
            z_copy(k, o).wait_send()

    for k in list(range(LOOK)) + [nk]:
        z_start(k)
    for k in range(LOOK, nk):
        fold(k)
    acc[...] = jnp.zeros_like(acc)

    def build(g):
        own = pl.ds(ex * jl, jl)
        lane = lax.broadcasted_iota(jnp.int32, (jl, LANES), 1)
        codes = [mbuf[g // 4, g % 4, zz, 0, own, :] for zz in range(ns)]
        gates_z = [mbuf[g // 4, g % 4, zz, 1, own, :] for zz in range(ns)]
        rew = [
            jnp.sum(jnp.where(lane == LANES - 1, b, 0.0), axis=1, keepdims=True) for b in codes
        ]
        total = rew[0]
        for r in rew[1:]:
            total = total + r
        wide = -(-kl // LANES) * LANES

        def along(blocks):
            out = jnp.zeros((jl, wide), F32)
            for zz, b in enumerate(blocks):
                b = jnp.where(lane < rows, b, 0.0)
                b = jnp.concatenate([b, jnp.zeros((jl, wide - LANES), F32)], axis=1)
                out = out + (pltpu.roll(b, zz * rows, 1) if zz else b)
            return out[:, :kl]

        vec = along(codes)
        scales = along(
            [b * -(rew[i] - (total - rew[i]) / (ns - 1)) for i, b in enumerate(gates_z)]
        )
        slots = NSUB * jl * cap_line
        ids = lax.broadcasted_iota(jnp.int32, (slots, kl), 0).astype(F32) + 1.0
        one = jnp.zeros((slots, kl), F32)
        scale = jnp.zeros((slots, kl), F32)
        for j in range(jl):
            same = ids == vec[j : j + 1]
            one = jnp.where(same, 1.0, one)
            scale = jnp.where(same, scales[j : j + 1], scale)
        one = one.astype(BF16)
        sel[g] = one
        scol[g] = jnp.sum(scale, axis=1, keepdims=True)
        sel_t[g] = dot_nt(eye(kl), one).astype(BF16)

    def select(k, scaled):
        for g in range(8):
            rowsv = buf[k, g // 4, g % 4].reshape(kl, cw)
            out = dot_nn(sel[g], rowsv)
            if scaled:
                out = out * scol[g]
            for s in range(NSUB):
                for j in range(jl):
                    r = (s * jl + j) * cap_line
                    xq[j, g * cap_line : (g + 1) * cap_line, s * cw : (s + 1) * cw] = out[
                        r : r + cap_line
                    ]
        xs[k] = xq[...].astype(BF16)

    def accumulate(i, slot, k):
        half = h // 2
        for j in range(jl):
            for r in (slice(0, half), slice(half, h)):
                acc[i, j, r] += dot_nt(wslot[slot, j, r], xs[k, j])

    def wait_w(slot):
        load(wg, 0, slot).wait()

    def step(i):
        @pl.when(i < nk - LOOK)
        def _():
            z_start(i + LOOK)

        @pl.when(i < nk)
        def _():
            stage_a(i)

        for fn, lag in zip((stage_b, stage_c, stage_d), AHEAD):

            @pl.when((i >= lag) & (i < nk + lag))
            def _():
                fn(i - lag)

    first = AHEAD[-1]
    stage_a(nk)
    step(0)
    stage_b(nk)
    step(1)
    stage_c(nk)
    step(2)
    stage_d(nk)
    lax.fori_loop(3, first, lambda i, _: (step(i), 0)[1], 0)
    lax.fori_loop(0, 8, lambda g, _: (build(g), 0)[1], 0)

    def token_chunk(q, _):
        step(q + first)
        select(q, False)
        s = 2 * (q % 2)
        wait_w(s)
        accumulate(0, s, q)
        wait_w(s + 1)
        accumulate(1, s + 1, q)

        @pl.when(q < NQ - 2)
        def _():
            load(wg, q + 2, s).start()
            load(wu, q + 2, s + 1).start()

        return 0

    lax.fori_loop(0, NQ, token_chunk, 0)

    def cot_chunk(q, _):
        step(q + NQ + first)
        select(q + NQ, True)
        s = 4 + q % 2
        wait_w(s)
        accumulate(2, s, q + NQ)

        @pl.when(q < NQ - 2)
        def _():
            load(wd, q + 2, s).start()

        @pl.when(q == NQ - 2)
        def _():
            load(wg, 1, s).start()

        @pl.when(q == NQ - 1)
        def _():
            load(wu, 1, s).start()

        return 0

    lax.fori_loop(0, NQ, cot_chunk, 0)

    def finish(t, _):
        tile = h // 4
        j = t // 4
        r = pl.ds(pl.multiple_of((t % 4) * tile, tile), tile)
        g, u, gh = acc[0, j, r], acc[1, j, r], acc[2, j, r]
        act, der = silu_parts(g)
        ht[0, j, r] = (act * u).astype(BF16)
        ht[1, j, r] = (gh * u * der).astype(BF16)
        ht[2, j, r] = (gh * act).astype(BF16)
        return 0

    lax.fori_loop(0, 4 * jl, finish, 0)

    def turn(t, _):
        gn[t // jl, t % jl] = dot_nt(eye(m), ht[1 + t // jl, t % jl]).astype(BF16)
        return 0

    lax.fori_loop(0, 2 * jl, turn, 0)
    outs = [
        pltpu.make_async_copy(ht.at[0], h_out, osem.at[0]),
        pltpu.make_async_copy(ht.at[1], gg_out, osem.at[1]),
        pltpu.make_async_copy(ht.at[2], gu_out, osem.at[2]),
        pltpu.make_async_copy(xs, x_out, osem.at[3]),
    ]
    for o in outs:
        o.start()

    def drain_all(k, _):
        drain(k)
        return 0

    lax.fori_loop(0, nk, drain_all, 0)
    drain(nk)

    def parts(i):
        q = NQ - 1 - i
        s = (2 - 2 * i + 12) % 6

        @pl.when(i >= 2)
        def _():
            wait_w(s)
            wait_w(s + 1)

        for j in range(jl):
            xq[j] = dot_nn(gn[0, j], wslot[s, j]) + dot_nn(gn[1, j], wslot[s + 1, j])

        @pl.when(i == 0)
        def _():
            load(wg, 0, s).start()
            load(wu, 0, s + 1).start()

        for g in range(8):
            at = slice(g * cap_line, (g + 1) * cap_line)
            pieces = [
                xq[j, at, sb * cw : (sb + 1) * cw] for sb in range(NSUB) for j in range(jl)
            ]
            v = jnp.concatenate(pieces, axis=0).astype(BF16)
            o = dot_nn(sel_t[g], v).astype(BF16)
            buf[q, g // 4, g % 4] = o.reshape(ns, rows, cw)

        send_core(q).start()

    def send_core(q):
        return rc(buf.at[q, 1 - c], r0.at[q], a_send.at[q], a_recv.at[q], dc)

    def send_far(q, i):
        return rc(
            buf.at[q, c, (l2, l3)[i]], r1.at[q, i], b_send.at[q, i], b_recv.at[q, i], d2
        )

    def send_near(q):
        return rc(buf.at[q, c, l1], r2.at[q], c_send.at[q], c_recv.at[q], d1)

    def send_z(q, o):
        to = dev(x, y, c, zpeer(o))
        return rc(buf.at[q, c, l0, zpeer(o)], r3.at[q, o], e_send.at[q, o], e_recv.at[q, o], to)

    def s1(q):
        send_core(q).wait_recv()
        for i, ll in ((0, l2), (1, l3)):
            buf[q, c, ll] = (buf[q, c, ll].astype(F32) + r0[q, ll].astype(F32)).astype(BF16)
            send_far(q, i).start()
        for ll in (l0, l1):
            buf[q, c, ll] = (buf[q, c, ll].astype(F32) + r0[q, ll].astype(F32)).astype(BF16)

    def s2(q):
        send_far(q, 1).wait_recv()
        buf[q, c, l1] = (buf[q, c, l1].astype(F32) + r1[q, 1].astype(F32)).astype(BF16)
        send_near(q).start()
        send_far(q, 0).wait_recv()
        buf[q, c, l0] = (buf[q, c, l0].astype(F32) + r1[q, 0].astype(F32)).astype(BF16)

    def s3(q):
        send_near(q).wait_recv()
        buf[q, c, l0] = (buf[q, c, l0].astype(F32) + r2[q].astype(F32)).astype(BF16)
        for o in range(1, ns):
            send_z(q, o).start()

    def s4(q):
        total = buf[q, c, l0, z].astype(F32)
        for o in range(1, ns):
            send_z(q, o).wait_recv()
            total = total + r3[q, o].astype(F32)
        total = total.astype(BF16)
        for sub in range(NSUB):
            at = pl.ds(pl.multiple_of(q * cq + sub * cw, cw), cw)
            gt[:, at] = dot_nn(take(rows, t, sub), total).astype(BF16)

    lags = cfg["lags"]

    def back_step(i, _):
        @pl.when(i < NQ)
        def _():
            parts(i)

        for fn, lag in zip((s1, s2, s3, s4), lags):

            @pl.when((i >= lag) & (i < lag + NQ))
            def _():
                fn(NQ - 1 - (i - lag))

        return 0

    lax.fori_loop(0, NQ + lags[-1], back_step, 0)

    def finish_sends(q, _):
        send_core(q).wait_send()
        send_far(q, 0).wait_send()
        send_far(q, 1).wait_send()
        send_near(q).wait_send()
        for o in range(1, ns):
            send_z(q, o).wait_send()
        return 0

    lax.fori_loop(0, NQ, finish_sends, 0)
    for o in outs:
        o.wait()


def weight_kernel(
    ht, gg, gu, xs, back, o_gate, o_up, o_down, o_back, hv, xv, stage, hsem, xsem, osem
):
    jl = ht.shape[0]
    cq = xs.shape[3]
    o_back[...] = back[...]
    lefts = (gg, gu, ht)
    dests = (o_gate, o_up, o_down)

    def left(i, j):
        return pltpu.make_async_copy(lefts[i].at[j], hv.at[i, j], hsem.at[i, j])

    def right(k):
        return pltpu.make_async_copy(xs.at[k], xv.at[k], xsem.at[k])

    def put(q, j, i):
        at = pl.ds(pl.multiple_of(q * cq, cq), cq)
        slot = q % 2
        return pltpu.make_async_copy(
            stage.at[slot, j, i], dests[i].at[j, :, at], osem.at[slot, j, i]
        )

    left(0, 0).start()
    right(0).start()
    left(1, 0).start()
    left(2, 0).start()
    right(NQ).start()
    for i in range(3):
        left(i, 1).start()
    for q in range(1, NQ):
        right(q).start()
        right(NQ + q).start()

    def step(q, _):
        for j in range(jl):
            for i in range(3):
                if i != 1 and j == 0:
                    right(q if i == 0 else NQ + q).wait()

                @pl.when(q == 0)
                def _():
                    left(i, j).wait()

                @pl.when(q >= 2)
                def _():
                    put(q - 2, j, i).wait()

                k = NQ + q if i == 2 else q
                stage[q % 2, j, i] = dot_nn(hv[i, j], xv[k, j]).astype(BF16)
                put(q, j, i).start()
        return 0

    lax.fori_loop(0, NQ, step, 0)
    for q in (NQ - 2, NQ - 1):
        for j in range(jl):
            for i in range(3):
                put(q, j, i).wait()


def fused(tokens, cotangent, routes, gate_weights, lengths, rewards, w_gate, w_up, w_down):
    ns = lax.axis_size("sample")
    t, d = tokens.shape
    jl, h, _ = w_gate.shape
    experts = jl * lax.axis_size("expert")
    rows = NSUB * t
    cw = d // (NSUB * NQ)
    cq = NSUB * cw
    cap_line = ns * CAP
    lines = 4
    m = 2 * lines * cap_line
    nk = 2 * NQ
    kl = ns * rows
    slots = NSUB * jl * cap_line
    cfg = dict(
        ns=ns, rows=rows, cw=cw, m=m, h=h, jl=jl, cap_line=cap_line, lags=(1, 3, 4, 6)
    )

    vmem = pl.BlockSpec(memory_space=pltpu.VMEM)
    hbm = pl.BlockSpec(memory_space=pltpu.HBM)
    dma = pltpu.SemaphoreType.DMA
    block = (rows, cw)
    back, ht, gg, gu, xs = pl.pallas_call(
        functools.partial(fused_kernel, cfg),
        name="gather_experts_scatter",
        out_shape=(
            jax.ShapeDtypeStruct((t, d), BF16),
            jax.ShapeDtypeStruct((jl, h, m), BF16),
            jax.ShapeDtypeStruct((jl, h, m), BF16),
            jax.ShapeDtypeStruct((jl, h, m), BF16),
            jax.ShapeDtypeStruct((nk, jl, m, cq), BF16),
        ),
        in_specs=[vmem] * 6 + [hbm] * 3,
        out_specs=(vmem, hbm, hbm, hbm, hbm),
        scratch_shapes=[
            pltpu.VMEM((nk, 2, lines, ns) + block, BF16),
            pltpu.VMEM((2, lines, ns, 2, experts, LANES), F32),
            pltpu.VMEM((NQ, lines, ns) + block, BF16),
            pltpu.VMEM((NQ, 2, ns) + block, BF16),
            pltpu.VMEM((NQ, ns) + block, BF16),
            pltpu.VMEM((NQ, ns) + block, BF16),
            pltpu.VMEM((nk, jl, m, cq), BF16),
            pltpu.VMEM((jl, m, cq), F32),
            pltpu.VMEM((3, jl, h, m), F32),
            pltpu.VMEM((3, jl, h, m), BF16),
            pltpu.VMEM((2, jl, m, h), BF16),
            pltpu.VMEM((2 * lines, slots, kl), BF16),
            pltpu.VMEM((2 * lines, kl, slots), BF16),
            pltpu.VMEM((2 * lines, slots, 1), F32),
            pltpu.VMEM((6, jl, h, cq), BF16),
            dma((nk + 1, ns)), dma((nk + 1, ns)), dma((nk + 1, 7)), dma((nk + 1, 3)),
            dma((nk + 1, 4)), dma((NQ,)), dma((NQ,)), dma((NQ, 2)), dma((NQ, 2)),
            dma((NQ,)), dma((NQ,)), dma((NQ, ns)), dma((NQ, ns)), dma((6,)), dma((4,)),
        ],
        compiler_params=pltpu.CompilerParams(
            collective_id=0, has_side_effects=True, vmem_limit_bytes=67043328
        ),
    )(tokens, cotangent, routes.T, gate_weights.T, lengths, rewards, w_gate, w_up, w_down)

    shape = jax.ShapeDtypeStruct(w_gate.shape, BF16)
    g_gate, g_up, g_down, g_tok = pl.pallas_call(
        weight_kernel,
        name="weight_grads",
        out_shape=(shape, shape, shape, jax.ShapeDtypeStruct((t, d), BF16)),
        in_specs=[hbm] * 4 + [vmem],
        out_specs=(hbm, hbm, hbm, vmem),
        scratch_shapes=[
            pltpu.VMEM((3, jl, h, m), BF16),
            pltpu.VMEM((nk, jl, m, cq), BF16),
            pltpu.VMEM((2, jl, 3, h, cq), BF16),
            dma((3, jl)), dma((nk,)), dma((2, jl, 3)),
        ],
        compiler_params=pltpu.CompilerParams(vmem_limit_bytes=67043328),
    )(ht, gg, gu, xs, back)
    return g_tok, g_gate, g_up, g_down


def covered(mesh, tokens_shape, w_shape, rewards_shape):
    nx, ne, ns = (mesh.shape[a] for a in ("dp", "expert", "sample"))
    t = tokens_shape[0] // (nx * ne * ns)
    d = tokens_shape[1]
    h = w_shape[1] // (nx * ns)
    prompt_one = rewards_shape == (nx * ne, ns)
    return (
        nx == 2
        and ne == 4
        and w_shape[0] == 2 * ne
        and prompt_one
        and ns > 1
        and (ns * CAP) % 8 == 0
        and (NSUB * t) % 16 == 0
        and NSUB * t < LANES
        and d % (NSUB * NQ * LANES) == 0
        and h % 1024 == 0
        and ns * t * d * h <= 80 * 4096 * 1024
    )


def solution(mesh):
    in_specs = (
        P(("dp", "expert", "sample"), None),
        P(("dp", "expert", "sample"), None),
        P(("dp", "expert", "sample"), None),
        P(("dp", "expert", "sample"), None),
        P(("dp", "expert"), "sample"),
        P(("dp", "expert"), "sample"),
        P("expert", ("dp", "sample"), None),
        P("expert", ("dp", "sample"), None),
        P("expert", ("dp", "sample"), None),
    )
    out_specs = (
        P(("dp", "expert", "sample"), None),
        P("expert", ("dp", "sample"), None),
        P("expert", ("dp", "sample"), None),
        P("expert", ("dp", "sample"), None),
    )

    def run(*args):
        fits = covered(mesh, args[0].shape, args[6].shape, args[5].shape)
        body = fused if fits else local
        return jax.shard_map(
            body, mesh=mesh, in_specs=in_specs, out_specs=out_specs, check_vma=False
        )(*args)

    return run
```

```python
import functools

import jax
import jax.numpy as jnp
from jax import lax
from jax.experimental import pallas as pl
from jax.experimental.pallas import tpu as pltpu
from jax.sharding import PartitionSpec as P

CAP = 6
BF16 = jnp.bfloat16
F32 = jnp.float32
MESH = pl.DeviceIdType.MESH


def silu_parts(pre_gate):
    gate_prob = jax.nn.sigmoid(pre_gate)
    return (pre_gate * gate_prob, gate_prob * (1.0 + pre_gate * (1.0 - gate_prob)))


def expert_rows(inputs, grads_out, w_gate, w_up, w_down):
    pre_gate = jnp.einsum("rjcd,jfd->rjcf", inputs, w_gate, preferred_element_type=jnp.float32)
    pre_up = jnp.einsum("rjcd,jfd->rjcf", inputs, w_up, preferred_element_type=jnp.float32)
    active, derivative = silu_parts(pre_gate)
    hidden = (active * pre_up).astype(jnp.bfloat16)
    grad_hidden = jnp.einsum(
        "rjcd,jfd->rjcf", grads_out, w_down, preferred_element_type=jnp.float32
    )
    grad_gate = (grad_hidden * pre_up * derivative).astype(jnp.bfloat16)
    grad_up = (grad_hidden * active).astype(jnp.bfloat16)
    return (hidden, grad_gate, grad_up)


def weight_terms(inputs, grads_out, hidden, grad_gate, grad_up):
    term_gate = jnp.einsum("rjcf,rjcd->jfd", grad_gate, inputs, preferred_element_type=jnp.float32)
    term_up = jnp.einsum("rjcf,rjcd->jfd", grad_up, inputs, preferred_element_type=jnp.float32)
    term_down = jnp.einsum("rjcf,rjcd->jfd", hidden, grads_out, preferred_element_type=jnp.float32)
    return (term_gate, term_up, term_down)


def input_terms(grad_gate, grad_up, w_gate, w_up):
    from_gate = jnp.einsum("rjcf,jfd->rjcd", grad_gate, w_gate, preferred_element_type=jnp.float32)
    from_up = jnp.einsum("rjcf,jfd->rjcd", grad_up, w_up, preferred_element_type=jnp.float32)
    return from_gate + from_up


def send_sum(blocks, axis):
    count = lax.axis_size(axis)
    me = lax.axis_index(axis)
    total = lax.dynamic_index_in_dim(blocks, me, 0, keepdims=False).astype(jnp.float32)
    for step in range(1, count):
        outgoing = lax.dynamic_index_in_dim(blocks, (me + step) % count, 0, keepdims=False)
        perm = [(i, (i + step) % count) for i in range(count)]
        total = total + lax.ppermute(outgoing, axis, perm).astype(jnp.float32)
    return total.astype(jnp.bfloat16)


def local(tokens, cotangent, routes, gate_weights, lengths, rewards, w_gate, w_up, w_down):
    samples = lax.axis_size("sample")
    own_reward = rewards.astype(jnp.float32) * 0.0625
    reward_total = own_reward
    for step in range(1, samples):
        perm = [(i, (i + step) % samples) for i in range(samples)]
        reward_total = reward_total + lax.ppermute(own_reward, "sample", perm)
    advantage = own_reward - (reward_total - own_reward) / (samples - 1)
    token_count = tokens.shape[0]
    model_width = tokens.shape[1]
    choices_per = routes.shape[1]
    local_experts = w_gate.shape[0]
    expert_groups = lax.axis_size("expert")
    all_experts = local_experts * expert_groups
    positions = jnp.arange(token_count, dtype=jnp.int32)
    weight_row = jnp.where(positions < lengths[0, 0], -advantage[0, 0], jnp.zeros((), jnp.float32))
    pair_scale = (gate_weights * weight_row[:, None]).reshape(-1)
    pair_expert = routes.reshape(-1)
    member = (pair_expert[:, None] == jnp.arange(all_experts, dtype=jnp.int32)[None, :]).astype(
        jnp.int32
    )
    earlier = jnp.sum((jnp.cumsum(member, axis=0) - member) * member, axis=1)
    target = pair_expert * CAP + earlier
    slot_ids = jnp.arange(all_experts * CAP, dtype=jnp.int32)
    placed = target[:, None] == slot_ids[None, :]
    chosen = jnp.sum(
        placed.reshape(token_count, choices_per, -1).astype(jnp.float32), axis=1
    ).astype(jnp.bfloat16)
    slot_scale = jnp.sum(jnp.where(placed, pair_scale[:, None], jnp.zeros((), jnp.float32)), axis=0)
    sent_inputs = jnp.dot(chosen.T, tokens, preferred_element_type=jnp.float32).astype(jnp.bfloat16)
    sent_cotangent = jnp.dot(chosen.T, cotangent, preferred_element_type=jnp.float32)
    sent_grads = (sent_cotangent * slot_scale[:, None]).astype(jnp.bfloat16)
    layout = (expert_groups, local_experts, CAP, model_width)
    arrived_inputs, arrived_grads = (
        lax.all_to_all(
            sent_inputs.reshape(layout), "expert", split_axis=0, concat_axis=0, tiled=True
        ),
        lax.all_to_all(
            sent_grads.reshape(layout), "expert", split_axis=0, concat_axis=0, tiled=True
        ),
    )
    group_inputs, group_grads = (
        lax.all_gather(arrived_inputs, ("dp", "sample"), axis=0, tiled=True),
        lax.all_gather(arrived_grads, ("dp", "sample"), axis=0, tiled=True),
    )
    hidden, grad_gate, grad_up = expert_rows(group_inputs, group_grads, w_gate, w_up, w_down)
    term_gate, term_up, term_down = weight_terms(
        group_inputs, group_grads, hidden, grad_gate, grad_up
    )
    parts = input_terms(grad_gate, grad_up, w_gate, w_up).astype(jnp.bfloat16)
    dp_size = lax.axis_size("dp")
    parts = parts.reshape(dp_size, samples, all_experts * CAP, model_width)
    row_sums = send_sum(send_sum(parts, "dp"), "sample").reshape(layout)
    returned = lax.all_to_all(row_sums, "expert", split_axis=0, concat_axis=0, tiled=True)
    flat_back = returned.reshape(all_experts * CAP, model_width)
    grad_tokens = jnp.dot(chosen, flat_back, preferred_element_type=jnp.float32).astype(
        jnp.bfloat16
    )
    return (
        grad_tokens,
        term_gate.astype(jnp.bfloat16),
        term_up.astype(jnp.bfloat16),
        term_down.astype(jnp.bfloat16),
    )


NSUB = 4
NQ = 4
LANES = 128
AHEAD = (2, 4, 5)
LOOK = 2


def dot_nt(a, b):
    return lax.dot_general(a, b, (((1,), (1,)), ((), ())), preferred_element_type=F32)


def dot_nn(a, b):
    return lax.dot_general(a, b, (((1,), (0,)), ((), ())), preferred_element_type=F32)


def eye(n):
    rows = lax.broadcasted_iota(jnp.int32, (n, n), 0)
    cols = lax.broadcasted_iota(jnp.int32, (n, n), 1)
    return jnp.where(rows == cols, 1.0, 0.0).astype(BF16)


def pack_meta(routes, gate_weights, lengths, rewards, experts, jl, cap_line, z):
    t = routes.shape[1]
    eid = lax.broadcasted_iota(jnp.int32, (experts, t), 0)
    live = lax.broadcasted_iota(jnp.int32, (1, t), 1) < lengths
    member = jnp.zeros((experts, t), F32)
    gate = jnp.zeros((experts, t), F32)
    for k in range(routes.shape[0]):
        hit = routes[k : k + 1] == eid
        member = jnp.where(hit, 1.0, member)
        gate = jnp.where(hit & live, gate_weights[k : k + 1], gate)
    before = lax.broadcasted_iota(jnp.int32, (t, t), 0) < lax.broadcasted_iota(jnp.int32, (t, t), 1)
    rank = dot_nn(member.astype(BF16), jnp.where(before, 1.0, 0.0).astype(BF16))
    base = ((eid % jl) * cap_line + z * CAP + 1).astype(F32)
    code = jnp.where(member > 0.0, rank + base, 0.0)
    reward = rewards.astype(F32) * 0.0625
    lanes = lax.broadcasted_iota(jnp.int32, (experts, LANES), 1)

    def spread(a, step):
        a = jnp.concatenate([a, jnp.zeros((experts, LANES - t), F32)], axis=1)
        out = a
        for sub in range(1, NSUB):
            moved = pltpu.roll(a, sub * t, 1)
            out = out + (jnp.where(moved > 0.0, moved + sub * step, 0.0) if step else moved)
        return jnp.where(lanes == LANES - 1, reward, out)

    return spread(code, float(jl * cap_line)), spread(gate, 0.0)


def place(rows, t, sub):
    r = lax.broadcasted_iota(jnp.int32, (rows, t), 0)
    i = lax.broadcasted_iota(jnp.int32, (rows, t), 1)
    return jnp.where(r == i + sub * t, 1.0, 0.0).astype(BF16)


def take(rows, t, sub):
    r = lax.broadcasted_iota(jnp.int32, (t, rows), 1)
    i = lax.broadcasted_iota(jnp.int32, (t, rows), 0)
    return jnp.where(r == i + sub * t, 1.0, 0.0).astype(BF16)


def fused_kernel(
    cfg,
    tok, cot, routes, gates, lengths, rewards, wg, wu, wd,
    gt, h_out, gg_out, gu_out, x_out,
    buf, mbuf, r0, r1, r2, r3, xs, xq, acc, ht, gn, sel, sel_t, scol, wslot,
    z_send, z_recv, l_send, l_recv, d_recv, a_send, a_recv, b_send, b_recv,
    c_send, c_recv, e_send, e_recv, wsem, osem,
):
    ns, rows, cw, m, h, jl, cap_line = (
        cfg["ns"], cfg["rows"], cfg["cw"], cfg["m"], cfg["h"], cfg["jl"], cfg["cap_line"]
    )
    nk = 2 * NQ
    cq = NSUB * cw
    kl = ns * rows
    x = lax.axis_index("dp")
    ex = lax.axis_index("expert")
    z = lax.axis_index("sample")
    y = ex // 2
    c = ex % 2
    x1, y1 = x + (1 - c) * (1 - 2 * x), y + c * (1 - 2 * y)
    x2, y2 = x + c * (1 - 2 * x), y + (1 - c) * (1 - 2 * y)
    l0 = x * 2 + y
    l1 = x1 * 2 + y1
    l2 = x2 * 2 + y2
    l3 = (1 - x) * 2 + (1 - y)

    def dev(xx, yy, cc, zz):
        return {"dp": xx, "expert": yy * 2 + cc, "sample": zz}

    d1, d2, dc = dev(x1, y1, c, z), dev(x2, y2, c, z), dev(x, y, 1 - c, z)

    def zpeer(o):
        return (z + o) % ns

    def zsrc(o):
        return (z - o + ns) % ns

    barrier = pltpu.get_barrier_semaphore()
    peers = [d1, d2, dc] + [dev(x, y, c, zpeer(o)) for o in range(1, ns)]
    for p in peers:
        pl.semaphore_signal(barrier, inc=1, device_id=p, device_id_type=MESH)

    def load(mat, q, slot):
        return pltpu.make_async_copy(
            mat.at[:, :, pl.ds(pl.multiple_of(q * cq, cq), cq)], wslot.at[slot], wsem.at[slot]
        )

    load(wg, 0, 0).start()
    load(wu, 0, 1).start()
    load(wg, 1, 2).start()
    load(wu, 1, 3).start()
    load(wd, 0, 4).start()
    load(wd, 1, 5).start()

    t = tok.shape[0]
    spots = [place(rows, t, sub) for sub in range(NSUB)]

    def fold(k):
        ref, q = (tok, k) if k < NQ else (cot, k - NQ)
        out = jnp.zeros((rows, cw), F32)
        for sub in range(NSUB):
            at = q * cq + sub * cw
            out = out + dot_nn(spots[sub], ref[:, at : at + cw])
        buf[k, c, l0, z] = out.astype(BF16)

    code, gate = pack_meta(
        routes[...], gates[...], lengths[...], rewards[...], mbuf.shape[4], jl, cap_line, z
    )
    mbuf[c, l0, z, 0] = code
    mbuf[c, l0, z, 1] = gate
    for k in range(LOOK):
        fold(k)
    pl.semaphore_wait(barrier, len(peers))

    def rc(src, dst, s, r, to):
        return pltpu.make_async_remote_copy(
            src_ref=src, dst_ref=dst, send_sem=s, recv_sem=r, device_id=to, device_id_type=MESH
        )

    def slab(k):
        return mbuf if isinstance(k, int) and k == nk else buf.at[k]

    def z_copy(k, o):
        b = slab(k).at[c, l0, z]
        return rc(b, b, z_send.at[k, o], z_recv.at[k, o], dev(x, y, c, zpeer(o)))

    def z_start(k):
        for o in range(1, ns):
            z_copy(k, o).start()

    def z_wait(k):
        for o in range(1, ns):
            b = slab(k).at[c, l0, zsrc(o)]
            rc(b, b, z_send.at[k, o], z_recv.at[k, o], d1).wait_recv()

    def line(k, cc, ll, si, r, to):
        b = slab(k).at[cc, ll]
        return rc(b, b, l_send.at[k, si], r, to)

    def stage_a(k):
        z_wait(k)
        line(k, c, l0, 0, l_recv.at[k, 0], d1).start()
        line(k, c, l0, 1, l_recv.at[k, 1], d2).start()
        line(k, c, l0, 2, d_recv.at[k, l0], dc).start()

    def stage_b(k):
        line(k, c, l1, 0, l_recv.at[k, 0], d1).wait_recv()
        line(k, c, l1, 3, l_recv.at[k, 2], d2).start()
        line(k, c, l1, 4, d_recv.at[k, l1], dc).start()

    def stage_c(k):
        line(k, c, l2, 1, l_recv.at[k, 1], d2).wait_recv()
        line(k, c, l2, 5, d_recv.at[k, l2], dc).start()
        line(k, c, l3, 3, l_recv.at[k, 2], d2).wait_recv()
        line(k, c, l3, 6, d_recv.at[k, l3], dc).start()

    def stage_d(k):
        for ll in range(4):
            line(k, 1 - c, ll, 2, d_recv.at[k, ll], dc).wait_recv()

    def drain(k):
        for i in range(7):
            line(k, c, l0, i, l_recv.at[k, 0], d1).wait_send()
        for o in range(1, ns):
            z_copy(k, o).wait_send()

    for k in list(range(LOOK)) + [nk]:
        z_start(k)
    for k in range(LOOK, nk):
        fold(k)
    acc[...] = jnp.zeros_like(acc)

    def build(g):
        own = pl.ds(ex * jl, jl)
        lane = lax.broadcasted_iota(jnp.int32, (jl, LANES), 1)
        codes = [mbuf[g // 4, g % 4, zz, 0, own, :] for zz in range(ns)]
        gates_z = [mbuf[g // 4, g % 4, zz, 1, own, :] for zz in range(ns)]
        rew = [
            jnp.sum(jnp.where(lane == LANES - 1, b, 0.0), axis=1, keepdims=True) for b in codes
        ]
        total = rew[0]
        for r in rew[1:]:
            total = total + r
        wide = -(-kl // LANES) * LANES

        def along(blocks):
            out = jnp.zeros((jl, wide), F32)
            for zz, b in enumerate(blocks):
                b = jnp.where(lane < rows, b, 0.0)
                b = jnp.concatenate([b, jnp.zeros((jl, wide - LANES), F32)], axis=1)
                out = out + (pltpu.roll(b, zz * rows, 1) if zz else b)
            return out[:, :kl]

        vec = along(codes)
        scales = along(
            [b * -(rew[i] - (total - rew[i]) / (ns - 1)) for i, b in enumerate(gates_z)]
        )
        slots = NSUB * jl * cap_line
        ids = lax.broadcasted_iota(jnp.int32, (slots, kl), 0).astype(F32) + 1.0
        one = jnp.zeros((slots, kl), F32)
        scale = jnp.zeros((slots, kl), F32)
        for j in range(jl):
            same = ids == vec[j : j + 1]
            one = jnp.where(same, 1.0, one)
            scale = jnp.where(same, scales[j : j + 1], scale)
        one = one.astype(BF16)
        sel[g] = one
        scol[g] = jnp.sum(scale, axis=1, keepdims=True)
        sel_t[g] = dot_nt(eye(kl), one).astype(BF16)

    def select(k, scaled):
        for g in range(8):
            rowsv = buf[k, g // 4, g % 4].reshape(kl, cw)
            out = dot_nn(sel[g], rowsv)
            if scaled:
                out = out * scol[g]
            for s in range(NSUB):
                for j in range(jl):
                    r = (s * jl + j) * cap_line
                    xq[j, g * cap_line : (g + 1) * cap_line, s * cw : (s + 1) * cw] = out[
                        r : r + cap_line
                    ]
        xs[k] = xq[...].astype(BF16)

    def accumulate(i, slot, k):
        half = h // 2
        for j in range(jl):
            for r in (slice(0, half), slice(half, h)):
                acc[i, j, r] += dot_nt(wslot[slot, j, r], xs[k, j])

    def wait_w(slot):
        load(wg, 0, slot).wait()

    def step(i):
        @pl.when(i < nk - LOOK)
        def _():
            z_start(i + LOOK)

        @pl.when(i < nk)
        def _():
            stage_a(i)

        for fn, lag in zip((stage_b, stage_c, stage_d), AHEAD):

            @pl.when((i >= lag) & (i < nk + lag))
            def _():
                fn(i - lag)

    first = AHEAD[-1]
    stage_a(nk)
    step(0)
    stage_b(nk)
    step(1)
    stage_c(nk)
    step(2)
    stage_d(nk)
    lax.fori_loop(3, first, lambda i, _: (step(i), 0)[1], 0)
    lax.fori_loop(0, 8, lambda g, _: (build(g), 0)[1], 0)

    def token_chunk(q, _):
        step(q + first)
        select(q, False)
        s = 2 * (q % 2)
        wait_w(s)
        accumulate(0, s, q)
        wait_w(s + 1)
        accumulate(1, s + 1, q)

        @pl.when(q < NQ - 2)
        def _():
            load(wg, q + 2, s).start()
            load(wu, q + 2, s + 1).start()

        return 0

    lax.fori_loop(0, NQ, token_chunk, 0)

    def cot_chunk(q, _):
        step(q + NQ + first)
        select(q + NQ, True)
        s = 4 + q % 2
        wait_w(s)
        accumulate(2, s, q + NQ)

        @pl.when(q < NQ - 2)
        def _():
            load(wd, q + 2, s).start()

        @pl.when(q == NQ - 2)
        def _():
            load(wg, 1, s).start()

        @pl.when(q == NQ - 1)
        def _():
            load(wu, 1, s).start()

        return 0

    lax.fori_loop(0, NQ, cot_chunk, 0)

    def finish(t, _):
        tile = h // 4
        j = t // 4
        r = pl.ds(pl.multiple_of((t % 4) * tile, tile), tile)
        g, u, gh = acc[0, j, r], acc[1, j, r], acc[2, j, r]
        act, der = silu_parts(g)
        ht[0, j, r] = (act * u).astype(BF16)
        ht[1, j, r] = (gh * u * der).astype(BF16)
        ht[2, j, r] = (gh * act).astype(BF16)
        return 0

    lax.fori_loop(0, 4 * jl, finish, 0)

    for i in range(2):
        for j in range(jl):
            gn[i, j] = dot_nt(eye(m), ht[1 + i, j]).astype(BF16)
    outs = [
        pltpu.make_async_copy(ht.at[0], h_out, osem.at[0]),
        pltpu.make_async_copy(ht.at[1], gg_out, osem.at[1]),
        pltpu.make_async_copy(ht.at[2], gu_out, osem.at[2]),
        pltpu.make_async_copy(xs, x_out, osem.at[3]),
    ]

    def drain_all(k, _):
        drain(k)
        return 0

    lax.fori_loop(0, nk, drain_all, 0)
    drain(nk)

    def parts(i):
        q = NQ - 1 - i
        s = (2 - 2 * i + 12) % 6

        @pl.when(i >= 2)
        def _():
            wait_w(s)
            wait_w(s + 1)

        for j in range(jl):
            xq[j] = dot_nn(gn[0, j], wslot[s, j]) + dot_nn(gn[1, j], wslot[s + 1, j])

        @pl.when(i == 0)
        def _():
            load(wg, 0, s).start()
            load(wu, 0, s + 1).start()

        for g in range(8):
            at = slice(g * cap_line, (g + 1) * cap_line)
            pieces = [
                xq[j, at, sb * cw : (sb + 1) * cw] for sb in range(NSUB) for j in range(jl)
            ]
            v = jnp.concatenate(pieces, axis=0).astype(BF16)
            o = dot_nn(sel_t[g], v).astype(BF16)
            buf[q, g // 4, g % 4] = o.reshape(ns, rows, cw)

        send_core(q).start()

    def send_core(q):
        return rc(buf.at[q, 1 - c], r0.at[q], a_send.at[q], a_recv.at[q], dc)

    def send_far(q, i):
        return rc(
            buf.at[q, c, (l2, l3)[i]], r1.at[q, i], b_send.at[q, i], b_recv.at[q, i], d2
        )

    def send_near(q):
        return rc(buf.at[q, c, l1], r2.at[q], c_send.at[q], c_recv.at[q], d1)

    def send_z(q, o):
        to = dev(x, y, c, zpeer(o))
        return rc(buf.at[q, c, l0, zpeer(o)], r3.at[q, o], e_send.at[q, o], e_recv.at[q, o], to)

    def s1(q):
        send_core(q).wait_recv()
        for i, ll in ((0, l2), (1, l3)):
            buf[q, c, ll] = (buf[q, c, ll].astype(F32) + r0[q, ll].astype(F32)).astype(BF16)
            send_far(q, i).start()
        for ll in (l0, l1):
            buf[q, c, ll] = (buf[q, c, ll].astype(F32) + r0[q, ll].astype(F32)).astype(BF16)

    def s2(q):
        send_far(q, 1).wait_recv()
        buf[q, c, l1] = (buf[q, c, l1].astype(F32) + r1[q, 1].astype(F32)).astype(BF16)
        send_near(q).start()
        send_far(q, 0).wait_recv()
        buf[q, c, l0] = (buf[q, c, l0].astype(F32) + r1[q, 0].astype(F32)).astype(BF16)

    def s3(q):
        send_near(q).wait_recv()
        buf[q, c, l0] = (buf[q, c, l0].astype(F32) + r2[q].astype(F32)).astype(BF16)
        for o in range(1, ns):
            send_z(q, o).start()

    def s4(q):
        total = buf[q, c, l0, z].astype(F32)
        for o in range(1, ns):
            send_z(q, o).wait_recv()
            total = total + r3[q, o].astype(F32)
        total = total.astype(BF16)
        for sub in range(NSUB):
            at = pl.ds(pl.multiple_of(q * cq + sub * cw, cw), cw)
            gt[:, at] = dot_nn(take(rows, t, sub), total).astype(BF16)

    lags = cfg["lags"]

    def back_step(i, _):
        @pl.when(i < NQ)
        def _():
            parts(i)

        @pl.when(i == NQ - 1)
        def _():
            for o in outs:
                o.start()

        for fn, lag in zip((s1, s2, s3, s4), lags):

            @pl.when((i >= lag) & (i < lag + NQ))
            def _():
                fn(NQ - 1 - (i - lag))

        return 0

    lax.fori_loop(0, NQ + lags[-1], back_step, 0)

    def finish_sends(q, _):
        send_core(q).wait_send()
        send_far(q, 0).wait_send()
        send_far(q, 1).wait_send()
        send_near(q).wait_send()
        for o in range(1, ns):
            send_z(q, o).wait_send()
        return 0

    lax.fori_loop(0, NQ, finish_sends, 0)
    for o in outs:
        o.wait()


def weight_kernel(
    ht, gg, gu, xs, back, o_gate, o_up, o_down, o_back, hv, xv, stage, hsem, xsem, osem
):
    jl = ht.shape[0]
    cq = xs.shape[3]
    o_back[...] = back[...]
    lefts = (gg, gu, ht)
    dests = (o_gate, o_up, o_down)

    def left(i, j):
        return pltpu.make_async_copy(lefts[i].at[j], hv.at[i, j], hsem.at[i, j])

    def right(k):
        return pltpu.make_async_copy(xs.at[k], xv.at[k], xsem.at[k])

    def put(q, j, i):
        at = pl.ds(pl.multiple_of(q * cq, cq), cq)
        slot = q % 2
        return pltpu.make_async_copy(
            stage.at[slot, j, i], dests[i].at[j, :, at], osem.at[slot, j, i]
        )

    left(0, 0).start()
    right(0).start()
    left(1, 0).start()
    left(2, 0).start()
    right(NQ).start()
    for i in range(3):
        left(i, 1).start()
    for q in range(1, NQ):
        right(q).start()
        right(NQ + q).start()

    def step(q, _):
        for j in range(jl):
            for i in range(3):
                if i != 1 and j == 0:
                    right(q if i == 0 else NQ + q).wait()

                @pl.when(q == 0)
                def _():
                    left(i, j).wait()

                @pl.when(q >= 2)
                def _():
                    put(q - 2, j, i).wait()

                k = NQ + q if i == 2 else q
                stage[q % 2, j, i] = dot_nn(hv[i, j], xv[k, j]).astype(BF16)
                put(q, j, i).start()
        return 0

    lax.fori_loop(0, NQ, step, 0)
    for q in (NQ - 2, NQ - 1):
        for j in range(jl):
            for i in range(3):
                put(q, j, i).wait()


def fused(tokens, cotangent, routes, gate_weights, lengths, rewards, w_gate, w_up, w_down):
    ns = lax.axis_size("sample")
    t, d = tokens.shape
    jl, h, _ = w_gate.shape
    experts = jl * lax.axis_size("expert")
    rows = NSUB * t
    cw = d // (NSUB * NQ)
    cq = NSUB * cw
    cap_line = ns * CAP
    lines = 4
    m = 2 * lines * cap_line
    nk = 2 * NQ
    kl = ns * rows
    slots = NSUB * jl * cap_line
    cfg = dict(
        ns=ns, rows=rows, cw=cw, m=m, h=h, jl=jl, cap_line=cap_line, lags=(1, 3, 4, 6)
    )

    vmem = pl.BlockSpec(memory_space=pltpu.VMEM)
    hbm = pl.BlockSpec(memory_space=pltpu.HBM)
    dma = pltpu.SemaphoreType.DMA
    block = (rows, cw)
    back, ht, gg, gu, xs = pl.pallas_call(
        functools.partial(fused_kernel, cfg),
        name="gather_experts_scatter",
        out_shape=(
            jax.ShapeDtypeStruct((t, d), BF16),
            jax.ShapeDtypeStruct((jl, h, m), BF16),
            jax.ShapeDtypeStruct((jl, h, m), BF16),
            jax.ShapeDtypeStruct((jl, h, m), BF16),
            jax.ShapeDtypeStruct((nk, jl, m, cq), BF16),
        ),
        in_specs=[vmem] * 6 + [hbm] * 3,
        out_specs=(vmem, hbm, hbm, hbm, hbm),
        scratch_shapes=[
            pltpu.VMEM((nk, 2, lines, ns) + block, BF16),
            pltpu.VMEM((2, lines, ns, 2, experts, LANES), F32),
            pltpu.VMEM((NQ, lines, ns) + block, BF16),
            pltpu.VMEM((NQ, 2, ns) + block, BF16),
            pltpu.VMEM((NQ, ns) + block, BF16),
            pltpu.VMEM((NQ, ns) + block, BF16),
            pltpu.VMEM((nk, jl, m, cq), BF16),
            pltpu.VMEM((jl, m, cq), F32),
            pltpu.VMEM((3, jl, h, m), F32),
            pltpu.VMEM((3, jl, h, m), BF16),
            pltpu.VMEM((2, jl, m, h), BF16),
            pltpu.VMEM((2 * lines, slots, kl), BF16),
            pltpu.VMEM((2 * lines, kl, slots), BF16),
            pltpu.VMEM((2 * lines, slots, 1), F32),
            pltpu.VMEM((6, jl, h, cq), BF16),
            dma((nk + 1, ns)), dma((nk + 1, ns)), dma((nk + 1, 7)), dma((nk + 1, 3)),
            dma((nk + 1, 4)), dma((NQ,)), dma((NQ,)), dma((NQ, 2)), dma((NQ, 2)),
            dma((NQ,)), dma((NQ,)), dma((NQ, ns)), dma((NQ, ns)), dma((6,)), dma((4,)),
        ],
        compiler_params=pltpu.CompilerParams(
            collective_id=0, has_side_effects=True, vmem_limit_bytes=67043328
        ),
    )(tokens, cotangent, routes.T, gate_weights.T, lengths, rewards, w_gate, w_up, w_down)

    shape = jax.ShapeDtypeStruct(w_gate.shape, BF16)
    g_gate, g_up, g_down, g_tok = pl.pallas_call(
        weight_kernel,
        name="weight_grads",
        out_shape=(shape, shape, shape, jax.ShapeDtypeStruct((t, d), BF16)),
        in_specs=[hbm] * 4 + [vmem],
        out_specs=(hbm, hbm, hbm, vmem),
        scratch_shapes=[
            pltpu.VMEM((3, jl, h, m), BF16),
            pltpu.VMEM((nk, jl, m, cq), BF16),
            pltpu.VMEM((2, jl, 3, h, cq), BF16),
            dma((3, jl)), dma((nk,)), dma((2, jl, 3)),
        ],
        compiler_params=pltpu.CompilerParams(vmem_limit_bytes=67043328),
    )(ht, gg, gu, xs, back)
    return g_tok, g_gate, g_up, g_down


def covered(mesh, tokens_shape, w_shape, rewards_shape):
    nx, ne, ns = (mesh.shape[a] for a in ("dp", "expert", "sample"))
    t = tokens_shape[0] // (nx * ne * ns)
    d = tokens_shape[1]
    h = w_shape[1] // (nx * ns)
    prompt_one = rewards_shape == (nx * ne, ns)
    return (
        nx == 2
        and ne == 4
        and w_shape[0] == 2 * ne
        and prompt_one
        and ns > 1
        and (ns * CAP) % 8 == 0
        and (NSUB * t) % 16 == 0
        and NSUB * t < LANES
        and d % (NSUB * NQ * LANES) == 0
        and h % 1024 == 0
        and ns * t * d * h <= 80 * 4096 * 1024
    )


def solution(mesh):
    in_specs = (
        P(("dp", "expert", "sample"), None),
        P(("dp", "expert", "sample"), None),
        P(("dp", "expert", "sample"), None),
        P(("dp", "expert", "sample"), None),
        P(("dp", "expert"), "sample"),
        P(("dp", "expert"), "sample"),
        P("expert", ("dp", "sample"), None),
        P("expert", ("dp", "sample"), None),
        P("expert", ("dp", "sample"), None),
    )
    out_specs = (
        P(("dp", "expert", "sample"), None),
        P("expert", ("dp", "sample"), None),
        P("expert", ("dp", "sample"), None),
        P("expert", ("dp", "sample"), None),
    )

    def run(*args):
        fits = covered(mesh, args[0].shape, args[6].shape, args[5].shape)
        body = fused if fits else local
        return jax.shard_map(
            body, mesh=mesh, in_specs=in_specs, out_specs=out_specs, check_vma=False
        )(*args)

    return run
```
